256 devices in a mesh: pa: 32 (over z, x), sa: 8 (over y, core).
Axes of the slice: x: 4, y: 4, z: 8, core: 2. Of those that a mesh axis runs over, the one named last changes fastest.
Arguments:
- factors: bfloat16 [64, 16, 4096], P(None, None, 'pa'), may hold values from -6 to 6
- trade_weights: bfloat16 [64, 8192], P(None, 'pa'), may hold values from -0.75 to 0.75
- payoff_terms: bfloat16 [2, 8192], P(None, 'pa'), may hold values from -6 to 6
- set_blocks: int32 [32], replicated, may hold values from 1 to 4, 64 in all
- shock_pick: int32 [16], P('sa'), may hold values from 0 to 31
- shock_scale: float32 [32, 64], replicated, may hold values from 0.25 to 1.75
- shock_shift: float32 [32, 64], replicated, may hold values from -3 to 3
- discount: bfloat16 [16, 4096], P(None, 'pa'), may hold values from 0.5 to 1
- set_pd: float32 [32, 16], P('pa'), may hold values from 0.02 to 0.2
- own_pd: float32 [16], replicated, may hold values from 0.02 to 0.2
Outputs:
- exposure_profile: float32 [2, 32, 16, 16], P(None, 'pa', None, 'sa')
- set_xva: float32 [32, 16], P('pa', 'sa')
- total_xva: float32 [16], P('sa')
The draws below stay inside these ranges and needn't reach their ends.
Inputs may be any that keep to these rules, and one draw needn't show every extreme that they name: `set_blocks`: each of the 32 netting sets holds whole consecutive blocks of 128 trades; the counts sum to 64.
All inputs are finite; a program needn't handle non-finite values.
Results may differ from the reference program's by a relative error of at most 0.00046.
Values may be sent and summed in bfloat16 or wider, within the bound.
A program may use at most 64 MiB of HBM per device.

```python
import math
import jax
import jax.numpy as jnp
import numpy as np
from jax import lax

K = 64
TRADES = 8192
TBLOCKS = 64
NSETS = 32
LIB = 32
DATES = 16
SHOCKS = 16
PATHS = 4096


def with_ends(values, key, smallest, top_value):
    dims = values.shape
    place = [jax.random.randint(jax.random.fold_in(key, axis), (), 0, dims[axis]) for axis in range(len(dims))]
    values = values.at[tuple(place)].set(smallest)
    longest = dims.index(max(dims))
    place[longest] = (place[longest] + 1) % dims[longest]
    return values.at[tuple(place)].set(top_value)


def shard_levels(stream_key, extent, pieces, low, high):
    loudness = 1.0
    for axis_at, shards_of in pieces:
        steps = jax.random.uniform(jax.random.fold_in(jax.random.fold_in(stream_key, 6), axis_at), (shards_of,), jnp.float32, low / len(pieces), high / len(pieces))
        loudness = loudness * jnp.repeat(jnp.exp(steps), extent[axis_at] // shards_of).reshape((-1,) + (1,) * (len(extent) - 1 - axis_at))
    return loudness


def split_up(number_of, total, most, skew):
    weights = [(1 << 20) // math.isqrt(rank ** skew) + 1 for rank in range(2, number_of + 1)]
    spare, holding = total - most - (number_of - 1), [1] * (number_of - 1)
    while spare > 0:
        candidates = [i for i in range(number_of - 1) if holding[i] < most]
        whole, left = sum([weights[i] for i in candidates]), spare
        for i in candidates:
            more = min(most - holding[i], max(1, left * weights[i] // whole), spare)
            holding[i] = holding[i] + more
            spare = spare - more
    return np.array([most] + holding)


def ragged(own_key, amount, total, reach, lean):
    if amount == 2:
        one = jax.random.randint(own_key, (), max(1, total - reach), min(reach, total - 1) + 1)
        return jnp.stack([one, total - one])
    lengths = jnp.asarray(split_up(amount, total, reach, lean), jnp.int32)
    pairs = (amount - 1) // 2
    donor, receiver = lengths[1:1 + 2 * pairs:2], lengths[2:2 + 2 * pairs:2]
    slack = jnp.minimum(donor - 1, reach - receiver)
    shifted = jax.random.randint(jax.random.fold_in(own_key, 1), (pairs,), 0, 1 << 20) % (slack + 1)
    lengths = lengths.at[1:1 + 2 * pairs:2].set(donor - shifted).at[2:2 + 2 * pairs:2].set(receiver + shifted)
    return lengths[jax.random.permutation(jax.random.fold_in(own_key, 2), amount)]


def gaussian(own_key, dims, scale, bound, pieces=(), kind=jnp.bfloat16):
    values = scale * jax.random.normal(own_key, dims, jnp.float32)
    if pieces:
        values = values * shard_levels(own_key, dims, pieces, -0.22, 0.18)
    return jnp.clip(values, -bound, bound).astype(kind)


def setup_inputs(seed: int = 0) -> dict:
    key_of = jax.random.split(jax.random.key(seed), 11)
    factors = gaussian(key_of[0], (K, DATES, PATHS), 1.0, 6.0, ((2, 32),))
    trade_weights = gaussian(key_of[1], (K, TRADES), K ** -0.5, 0.75, ((1, 32),))
    payoff_terms = gaussian(key_of[2], (2, TRADES), 1.0, 6.0, ((1, 32),))
    set_blocks = ragged(key_of[3], NSETS, TBLOCKS, 4, 2).astype(jnp.int32)
    shock_pick = with_ends(jax.random.randint(key_of[4], (SHOCKS,), 0, LIB), jax.random.fold_in(key_of[4], 1), 0, LIB - 1).astype(jnp.int32)
    shock_scale = jnp.clip(1.0 + 0.15 * jax.random.normal(key_of[5], (LIB, K), jnp.float32), 0.25, 1.75)
    shock_shift = gaussian(key_of[6], (LIB, K), 0.5, 3.0, (), jnp.float32)
    discount = jnp.clip(jnp.exp(math.log(1.0) - 0.6931472 * jax.random.uniform(key_of[7], (DATES, PATHS), jnp.float32) ** shard_levels(key_of[7], (DATES, PATHS), ((1, 32),), -0.2, 0.2)), 0.5, 1.0).astype(jnp.bfloat16)
    set_pd = jnp.clip(jnp.exp(math.log(0.2) - 2.3025851 * jax.random.uniform(key_of[8], (NSETS, DATES), jnp.float32) ** shard_levels(key_of[8], (NSETS, DATES), ((0, 32),), -0.2, 0.2)), 0.02, 0.2)
    own_pd = jnp.clip(jnp.exp(jax.random.uniform(key_of[9], (DATES,), jnp.float32, math.log(0.02), math.log(0.2))), 0.02, 0.2)
    return dict(factors=factors, trade_weights=trade_weights, payoff_terms=payoff_terms, set_blocks=set_blocks, shock_pick=shock_pick, shock_scale=shock_scale, shock_shift=shock_shift, discount=discount, set_pd=set_pd, own_pd=own_pd)


UNIT_SCALE = 0.0625


def trade_members(set_blocks):
    set_ends = jnp.cumsum(set_blocks).astype(jnp.int32)
    block_ids = jnp.arange(TBLOCKS, dtype=jnp.int32)
    owners = jnp.sum((set_ends[None, :] <= block_ids[:, None]).astype(jnp.int32), axis=1).astype(jnp.int32)
    trade_owner = jnp.repeat(owners, 128)
    set_ids = jnp.arange(NSETS, dtype=jnp.int32)
    return (trade_owner[None, :] == set_ids[:, None]).astype(jnp.bfloat16)


def reference(factors, trade_weights, payoff_terms, set_blocks, shock_pick, shock_scale, shock_shift, discount, set_pd, own_pd):
    members = trade_members(set_blocks)
    library = jnp.arange(LIB, dtype=jnp.int32)
    pick_rows = (shock_pick[:, None] == library[None, :]).astype(jnp.float32)
    scale_rows = jnp.dot(pick_rows, shock_scale, precision=lax.Precision.HIGHEST)
    shift_rows = jnp.dot(pick_rows, shock_shift, precision=lax.Precision.HIGHEST)
    notional = payoff_terms[0].astype(jnp.float32)[:, None]
    strike = payoff_terms[1].astype(jnp.float32)[:, None]

    def one_pair(position):
        date_index = position // SHOCKS
        shock_index = position % SHOCKS
        date_factors = lax.dynamic_index_in_dim(factors, date_index, 1, False).astype(jnp.float32)
        scale_one = lax.dynamic_index_in_dim(scale_rows, shock_index, 0, False)
        shift_one = lax.dynamic_index_in_dim(shift_rows, shock_index, 0, False)
        shocked = (scale_one[:, None] * date_factors + shift_one[:, None]).astype(jnp.bfloat16)
        levels = lax.dot_general(trade_weights, shocked, (((0,), (0,)), ((), ())), preferred_element_type=jnp.float32)
        values = (notional * jax.nn.softplus(levels + strike)).astype(jnp.bfloat16)
        netted = UNIT_SCALE * jnp.dot(members, values, preferred_element_type=jnp.float32)
        date_discount = lax.dynamic_index_in_dim(discount, date_index, 0, False).astype(jnp.float32)
        exposure = netted * date_discount[None, :]
        positive = jnp.sum(jnp.maximum(exposure, 0.0), axis=1) / PATHS
        negative = jnp.sum(jnp.minimum(exposure, 0.0), axis=1) / PATHS
        return jnp.stack([positive, negative])

    results = lax.map(one_pair, jnp.arange(DATES * SHOCKS, dtype=jnp.int32))
    profile = results.reshape(DATES, SHOCKS, 2, NSETS).transpose(2, 3, 0, 1)
    adjustment = jnp.sum(set_pd[:, :, None] * profile[0], axis=1) + jnp.sum(own_pd[None, :, None] * profile[1], axis=1)
    set_xva = adjustment - jnp.sum(adjustment, axis=1, keepdims=True) / SHOCKS
    total_xva = jnp.sum(adjustment, axis=0)
    return profile, set_xva, total_xva
```

```python
import functools

import jax
import jax.numpy as jnp
from jax import lax
from jax.experimental import pallas as pl
from jax.experimental.pallas import tpu as pltpu
from jax.sharding import PartitionSpec as P

BF = jnp.bfloat16
F32 = jnp.float32
K = 64
SETS = 32
DATES = 16
LANES = 128
ROWS = 80
GROUPS = 32
STEPS = 8
PIECE = 128
PIECES = 2
NZ, NX, NPA, NSA = 8, 4, 32, 8
LOG2E = 1.4426950408889634
LN2 = 0.6931471805599453
MESH = pl.DeviceIdType.MESH


def ring(delta, extent):
    return min(delta, extent - delta)


OFFSETS = sorted(
    ((dz, dx) for dz in range(NZ) for dx in range(NX)),
    key=lambda o: (ring(o[0], NZ) + ring(o[1], NX), ring(o[0], NZ), o[0] > NZ // 2, o[1]),
)


def shifted(me, offset):
    z, x = me // NX, lax.rem(me, NX)
    return lax.rem(z + offset[0], NZ) * NX + lax.rem(x + offset[1], NX)


def back(offset):
    return ((NZ - offset[0]) % NZ, (NX - offset[1]) % NX)


def parts_of(value):
    high = value.astype(BF).astype(F32)
    rest = value - high
    middle = rest.astype(BF).astype(F32)
    return high, middle, rest - middle


def kernel(
    blocks, pick, factors, weights, terms, scale, shift, discount, set_pd, own_pd,
    profile_out, xva_out, total_out,
    tiles, shocked, flat, sides, staged, members_ref, coef_row, coefs, sums, outbox, inbox, near_out, near_in,
    send_sems, tile_sems, out_sems, in_sems, near_send, near_recv,
):
    pa = lax.axis_index("pa")
    sa = lax.axis_index("sa")

    barrier = pltpu.get_barrier_semaphore()
    for offset in OFFSETS[1:]:
        pl.semaphore_signal(barrier, inc=1, device_id={"pa": shifted(pa, offset)}, device_id_type=MESH)
    for hop in range(1, NSA):
        pl.semaphore_signal(barrier, inc=1, device_id={"sa": lax.rem(sa + hop, NSA)}, device_id_type=MESH)

    coef_row[...] = jnp.zeros_like(coef_row)
    coef_row[0:1, 0:16] = set_pd[...]
    coef_row[0:1, 16:32] = set_pd[...]
    coef_row[0:1, 32:48] = own_pd[...]
    coef_row[0:1, 48:64] = own_pd[...]
    coef = coef_row[0:1, :]
    ends = []
    running = jnp.int32(0)
    for m in range(SETS):
        running = running + blocks[m]
        ends.append(running)
    row = lax.broadcasted_iota(jnp.int32, (16, LANES), 0)
    for half in range(2):
        block = 2 * pa + half
        owner = jnp.int32(0)
        for end in ends:
            owner = owner + jnp.where(end <= block, 1, 0).astype(jnp.int32)
        lanes = slice(half * LANES, (half + 1) * LANES)
        notional = terms[0:1, lanes].astype(F32)
        strike = parts_of(terms[1:2, lanes].astype(F32) * LOG2E)
        rows = [*strike, notional, jnp.full((1, LANES), owner.astype(F32))]
        if half == 0:
            rows.extend(parts_of(coef))
        block_rows = jnp.zeros((16, LANES), F32)
        for i, value in enumerate(rows):
            block_rows = jnp.where(row == i, value, block_rows)
        tiles[0, half, 0:K] = weights[:, lanes]
        tiles[0, half, K:ROWS] = block_rows.astype(BF)

    for k in range(K):
        flat[k * DATES:(k + 1) * DATES, :] = factors[k].astype(F32)
    ones = jnp.where(lax.broadcasted_iota(jnp.int32, (K, LANES), 0) < 3, 1.0, 0.0).astype(BF)
    none = jnp.zeros((K, LANES), BF)
    for s in range(2):
        which = pick[s]
        scales = jnp.broadcast_to(scale[pl.ds(which, 1), :], (LANES, K)).T
        shifts = jnp.broadcast_to(shift[pl.ds(which, 1), :], (LANES, K)).T
        for d in range(DATES):
            g = s * DATES + d
            base = flat[pl.ds(d, K, stride=DATES), :]
            value = (scales * base + shifts).astype(BF).astype(F32) * LOG2E
            high = value.astype(BF)
            shocked[g, 0:K] = high
            shocked[g, K:2 * K] = ones
            shocked[g, 2 * K:3 * K] = (value - high.astype(F32)).astype(BF)
            shocked[g, 3 * K:4 * K] = none

    pl.semaphore_wait(barrier, NPA - 1 + NSA - 1)

    def tile_copy(k, target):
        return pltpu.make_async_remote_copy(
            src_ref=tiles.at[0], dst_ref=tiles.at[k], send_sem=send_sems.at[k], recv_sem=tile_sems.at[k],
            device_id={"pa": target}, device_id_type=MESH,
        )

    for k in range(1, NPA):
        tile_copy(k, shifted(pa, back(OFFSETS[k]))).start()

    def members(s):
        halves = []
        for half in range(2):
            info = tiles[s, half, K:ROWS].astype(F32)
            ids = lax.broadcasted_iota(jnp.int32, (SETS, LANES), 0).astype(F32)
            halves.append(jnp.where(ids == info[4:5, :], info[3:4, :], 0.0).astype(BF))
        return jnp.concatenate(halves, 1)

    def prepare(s, slot):
        for half in range(2):
            tile = jnp.concatenate([tiles[s, half], jnp.zeros((LANES - ROWS, LANES), BF)], 0)
            sides[slot, half * LANES:(half + 1) * LANES] = tile.T

    def softplus2(x):
        y = lax.log2(1.0 + lax.exp2(jnp.minimum(x, 100.0)))
        return jnp.maximum(y, x).astype(BF)

    def body(levels, nets):
        def push_shocked(q, j):
            g = (2 * (j % STEPS) + q) * 2
            both = jnp.concatenate([shocked[g], shocked[g + 1]], 1)
            pltpu.matmul_push_rhs(both, staging_register=0, mxu_index=q)

        def level(q, j, p, slot):
            side = sides[slot, p * PIECE:(p + 1) * PIECE]
            pltpu.matmul_acc_lhs(
                levels[q][j % 2][p], jnp.concatenate([side, side], 1), load_staged_rhs=0 if p == 0 else None
            )

        def net(q, j, chosen):
            values = staged[q, j % 2]
            pltpu.matmul_push_rhs(jnp.concatenate([values[0], values[1]], 1), staging_register=1, mxu_index=q)
            pltpu.matmul_acc_lhs(nets[q][j], chosen, load_staged_rhs=1)

        for q in range(2):
            for acc in nets[q]:
                pltpu.matmul_pop(acc)
            for r in range(2):
                for p in range(PIECES):
                    pltpu.matmul_pop(levels[q][r][p])
        prepare(0, 0)
        for j in range(2):
            for q in range(2):
                push_shocked(q, j)
                for p in range(PIECES):
                    level(q, j, p, 0)
        members_ref[...] = jnp.zeros_like(members_ref)
        staged[...] = jnp.zeros_like(staged)

        def shard(s, carry):
            @pl.when(s < NPA - 1)
            def _():
                tile_copy(s + 1, pa).wait_recv()

            chosen = members(s)
            prepare(lax.min(s + 1, NPA - 1), (s + 1) % 2)
            for j in range(STEPS):
                slot = (s + (j + 2) // STEPS) % 2
                for q in range(2):
                    push_shocked(q, j + 2)
                for p in range(PIECES):
                    for q in range(2):
                        x = pltpu.matmul_pop(levels[q][j % 2][p])
                        level(q, j + 2, p, slot)
                        value = softplus2(x)
                        for h in range(2):
                            staged[q, j % 2, h, p * PIECE:(p + 1) * PIECE] = value[:, h * LANES:(h + 1) * LANES]
                for q in range(2):
                    net(q, (j - 1) % STEPS, chosen if j else members_ref[...])
            members_ref[...] = chosen
            return carry

        lax.fori_loop(0, NPA, shard, 0)
        for q in range(2):
            net(q, STEPS - 1, members_ref[...])
            for r in range(2):
                for p in range(PIECES):
                    pltpu.matmul_pop(levels[q][r][p])

        lane = lax.broadcasted_iota(jnp.int32, (SETS, LANES), 1)
        partial = jnp.zeros((SETS, LANES), F32)
        for j in range(STEPS):
            for q in range(2):
                netted = pltpu.matmul_pop(nets[q][j])
                for h in range(2):
                    g = (2 * j + q) * 2 + h
                    d = g % DATES
                    exposure = netted[:, h * LANES:(h + 1) * LANES] * (0.0625 * LN2) * discount[d:d + 1, :].astype(F32)
                    positive = jnp.sum(jnp.maximum(exposure, 0.0), axis=1, keepdims=True)
                    negative = jnp.sum(jnp.minimum(exposure, 0.0), axis=1, keepdims=True)
                    partial = jnp.where(lane == g, positive, partial)
                    partial = jnp.where(lane == GROUPS + g, negative, partial)
        sums[...] = partial

    acc = lambda q, m: pltpu.ACC(q)((m, 256), F32)
    pl.run_scoped(
        body,
        [[[acc(q, PIECE) for _ in range(PIECES)] for _ in range(2)] for q in range(2)],
        [[acc(q, SETS) for _ in range(STEPS)] for q in range(2)],
    )

    for k in range(NPA):
        info = tiles[k, 0, K:ROWS].astype(F32)
        coefs[pl.ds(shifted(pa, OFFSETS[k]), 1), :] = info[5:6, :] + info[6:7, :] + info[7:8, :]
    partial = sums[...] * (1.0 / (NPA * LANES))
    totals = jnp.sum(partial * coefs[...], axis=0, keepdims=True)
    rows = partial + pltpu.roll(jnp.broadcast_to(totals, (8, LANES)), 64, 1)[0:1, :]
    for n in range(SETS):
        outbox[n] = rows[n:n + 1, :]

    def row_copy(k, target):
        return pltpu.make_async_remote_copy(
            src_ref=outbox.at[target], dst_ref=inbox.at[k], send_sem=out_sems.at[k], recv_sem=in_sems.at[k],
            device_id={"pa": target}, device_id_type=MESH,
        )

    for k in range(NPA - 1, 0, -1):
        row_copy(k, shifted(pa, OFFSETS[k])).start()
    inbox[0] = outbox[pa]
    for k in range(1, NPA):
        row_copy(k, shifted(pa, OFFSETS[k])).wait_recv()
    mine = jnp.sum(inbox[...], axis=0)

    lane = lax.broadcasted_iota(jnp.int32, (1, LANES), 1)
    weighted = mine * coef
    first = lax.rem(lane // DATES, 2) == 0
    upper = lane >= 64

    def lane_sum(value, mask):
        return jnp.sum(jnp.where(mask, value, 0.0), axis=1, keepdims=True)

    adjust = [lane_sum(weighted, first), lane_sum(weighted, jnp.logical_not(first))]
    total = [
        lane_sum(mine, jnp.logical_and(first, upper)),
        lane_sum(mine, jnp.logical_and(jnp.logical_not(first), upper)),
    ]
    near_out[...] = jnp.broadcast_to(adjust[0] + adjust[1], (1, LANES))

    def near_copy(hop, target):
        return pltpu.make_async_remote_copy(
            src_ref=near_out, dst_ref=near_in.at[hop], send_sem=near_send.at[hop], recv_sem=near_recv.at[hop],
            device_id={"sa": target}, device_id_type=MESH,
        )

    for hop in range(1, NSA):
        near_copy(hop, lax.rem(sa + hop, NSA)).start()
    near_in[0] = near_out[...]

    columns = jnp.broadcast_to(mine, (8, LANES)).T
    pair = lax.broadcasted_iota(jnp.int32, (DATES, 2), 1) == 0
    for sign in range(2):
        low = columns[sign * 32:sign * 32 + 16, 0:2]
        high = columns[sign * 32 + 16:sign * 32 + 32, 0:2]
        profile_out[sign] = jnp.where(pair, low, high)
    two = lax.broadcasted_iota(jnp.int32, (1, 2), 1) == 0
    total_out[...] = jnp.where(two, total[0], total[1])

    for hop in range(1, NSA):
        near_copy(hop, lax.rem(sa + hop, NSA)).wait_recv()
    mean = jnp.sum(near_in[...], axis=0)[:, 0:1] / (2 * NSA)
    xva_out[...] = jnp.where(two, adjust[0] - mean, adjust[1] - mean)

    for k in range(1, NPA):
        tile_copy(k, pa).wait_send()
        row_copy(k, shifted(pa, OFFSETS[k])).wait_send()
    for hop in range(1, NSA):
        near_copy(hop, sa).wait_send()


def on_device(
    factors, trade_weights, payoff_terms, set_blocks, shock_pick, shock_scale, shock_shift, discount, set_pd, own_pd
):
    vmem = pl.BlockSpec(memory_space=pltpu.VMEM)
    smem = pl.BlockSpec(memory_space=pltpu.SMEM)
    profile, xva, total = pl.pallas_call(
        kernel,
        out_shape=(
            jax.ShapeDtypeStruct((2, DATES, 2), F32),
            jax.ShapeDtypeStruct((1, 2), F32),
            jax.ShapeDtypeStruct((1, 2), F32),
        ),
        in_specs=[smem, smem] + [vmem] * 8,
        out_specs=(vmem, vmem, vmem),
        scratch_shapes=[
            pltpu.VMEM((NPA, 2, ROWS, LANES), BF),
            pltpu.VMEM((GROUPS, 256, LANES), BF),
            pltpu.VMEM((K * DATES, LANES), F32),
            pltpu.VMEM((2, 256, LANES), BF),
            pltpu.VMEM((2, 2, 2, 256, LANES), BF),
            pltpu.VMEM((SETS, 256), BF),
            pltpu.VMEM((8, LANES), F32),
            pltpu.VMEM((SETS, LANES), F32),
            pltpu.VMEM((SETS, LANES), F32),
            pltpu.VMEM((SETS, 1, LANES), F32),
            pltpu.VMEM((NPA, 1, LANES), F32),
            pltpu.VMEM((1, LANES), F32),
            pltpu.VMEM((NSA, 1, LANES), F32),
            pltpu.SemaphoreType.DMA((NPA,)),
            pltpu.SemaphoreType.DMA((NPA,)),
            pltpu.SemaphoreType.DMA((NPA,)),
            pltpu.SemaphoreType.DMA((NPA,)),
            pltpu.SemaphoreType.DMA((NSA,)),
            pltpu.SemaphoreType.DMA((NSA,)),
        ],
        compiler_params=pltpu.CompilerParams(
            collective_id=0, has_side_effects=True, vmem_limit_bytes=24 << 20
        ),
        name="valuation",
    )(
        set_blocks, shock_pick, factors, trade_weights, payoff_terms, shock_scale, shock_shift, discount, set_pd,
        own_pd.reshape(1, DATES),
    )
    return profile.reshape(2, 1, DATES, 2), xva, total.reshape(2)


def solution(mesh):
    return jax.shard_map(
        on_device,
        mesh=mesh,
        in_specs=(
            P(None, None, "pa"), P(None, "pa"), P(None, "pa"), P(), P("sa"), P(), P(), P(None, "pa"),
            P("pa", None), P(),
        ),
        out_specs=(P(None, "pa", None, "sa"), P("pa", "sa"), P("sa")),
        check_vma=False,
    )
```

```python
import functools

import jax
import jax.numpy as jnp
from jax import lax
from jax.experimental import pallas as pl
from jax.experimental.pallas import tpu as pltpu
from jax.sharding import PartitionSpec as P

BF = jnp.bfloat16
F32 = jnp.float32
K = 64
SETS = 32
DATES = 16
LANES = 128
ROWS = 80
GROUPS = 32
STEPS = 8
PIECE = 128
PIECES = 2
NZ, NX, NPA, NSA = 8, 4, 32, 8
LOG2E = 1.4426950408889634
LN2 = 0.6931471805599453
MESH = pl.DeviceIdType.MESH


def ring(delta, extent):
    return min(delta, extent - delta)


OFFSETS = sorted(
    ((dz, dx) for dz in range(NZ) for dx in range(NX)),
    key=lambda o: (ring(o[0], NZ) + ring(o[1], NX), ring(o[0], NZ), o[0] > NZ // 2, o[1]),
)


def shifted(me, offset):
    z, x = me // NX, lax.rem(me, NX)
    return lax.rem(z + offset[0], NZ) * NX + lax.rem(x + offset[1], NX)


def back(offset):
    return ((NZ - offset[0]) % NZ, (NX - offset[1]) % NX)


def parts_of(value):
    high = value.astype(BF).astype(F32)
    rest = value - high
    middle = rest.astype(BF).astype(F32)
    return high, middle, rest - middle


def kernel(
    *refs,
):
    hbm, refs = refs[:10], refs[10:]
    result, refs = refs[0], refs[1:]
    local, refs = refs[:10], refs[10:]
    blocks, pick, factors, weights, terms, scale, shift, discount, set_pd, own_pd = local
    (
        tiles, shocked, flat, side0, side1, stage00, stage01, stage10, stage11, members_ref, coef_row, coefs, sums,
        outbox, inbox, near_out, near_in,
        load_sems, send_sems, tile_sems, out_sems, in_sems, near_send, near_recv,
    ) = refs
    sides = [side0, side1]
    staged = [[stage00, stage01], [stage10, stage11]]
    pa = lax.axis_index("pa")
    sa = lax.axis_index("sa")
    loads = [pltpu.make_async_copy(hbm[i], local[i], load_sems.at[i]) for i in range(10)]
    for load in loads:
        load.start()

    barrier = pltpu.get_barrier_semaphore()
    for offset in OFFSETS[1:]:
        pl.semaphore_signal(barrier, inc=1, device_id={"pa": shifted(pa, offset)}, device_id_type=MESH)
    for hop in range(1, NSA):
        pl.semaphore_signal(barrier, inc=1, device_id={"sa": lax.rem(sa + hop, NSA)}, device_id_type=MESH)

    for load in loads:
        load.wait()

    coef_row[...] = jnp.zeros_like(coef_row)
    coef_row[0:1, 0:16] = set_pd[...]
    coef_row[0:1, 16:32] = set_pd[...]
    coef_row[0:1, 32:48] = own_pd[...]
    coef_row[0:1, 48:64] = own_pd[...]
    coef = coef_row[0:1, :]
    ends = []
    running = jnp.int32(0)
    for m in range(SETS):
        running = running + blocks[m]
        ends.append(running)
    row = lax.broadcasted_iota(jnp.int32, (16, LANES), 0)
    for half in range(2):
        block = 2 * pa + half
        owner = jnp.int32(0)
        for end in ends:
            owner = owner + jnp.where(end <= block, 1, 0).astype(jnp.int32)
        lanes = slice(half * LANES, (half + 1) * LANES)
        notional = terms[0:1, lanes].astype(F32)
        strike = parts_of(terms[1:2, lanes].astype(F32) * LOG2E)
        rows = [*strike, notional, jnp.full((1, LANES), owner.astype(F32))]
        if half == 0:
            rows.extend(parts_of(coef))
        block_rows = jnp.zeros((16, LANES), F32)
        for i, value in enumerate(rows):
            block_rows = jnp.where(row == i, value, block_rows)
        tiles[0, half, 0:K] = weights[:, lanes]
        tiles[0, half, K:ROWS] = block_rows.astype(BF)

    for k in range(K):
        flat[k * DATES:(k + 1) * DATES, :] = factors[k].astype(F32)
    ones = jnp.where(lax.broadcasted_iota(jnp.int32, (K, LANES), 0) < 3, 1.0, 0.0).astype(BF)
    none = jnp.zeros((K, LANES), BF)
    for s in range(2):
        which = pick[s]
        scales = jnp.broadcast_to(scale[pl.ds(which, 1), :], (LANES, K)).T
        shifts = jnp.broadcast_to(shift[pl.ds(which, 1), :], (LANES, K)).T
        for d in range(DATES):
            g = s * DATES + d
            base = flat[pl.ds(d, K, stride=DATES), :]
            value = (scales * base + shifts).astype(BF).astype(F32) * LOG2E
            high = value.astype(BF)
            shocked[g, 0:K] = high
            shocked[g, K:2 * K] = ones
            shocked[g, 2 * K:3 * K] = (value - high.astype(F32)).astype(BF)
            shocked[g, 3 * K:4 * K] = none

    pl.semaphore_wait(barrier, NPA - 1 + NSA - 1)

    def tile_copy(k, target):
        return pltpu.make_async_remote_copy(
            src_ref=tiles.at[0], dst_ref=tiles.at[k], send_sem=send_sems.at[k], recv_sem=tile_sems.at[k],
            device_id={"pa": target}, device_id_type=MESH,
        )

    for k in range(1, NPA):
        tile_copy(k, shifted(pa, back(OFFSETS[k]))).start()

    def members(s):
        halves = []
        for half in range(2):
            info = tiles[s, half, K:ROWS].astype(F32)
            ids = lax.broadcasted_iota(jnp.int32, (SETS, LANES), 0).astype(F32)
            halves.append(jnp.where(ids == info[4:5, :], info[3:4, :], 0.0).astype(BF))
        return jnp.concatenate(halves, 1)

    def prepare(s, slot):
        for half in range(2):
            tile = jnp.concatenate([tiles[s, half], jnp.zeros((LANES - ROWS, LANES), BF)], 0)
            sides[slot][half * LANES:(half + 1) * LANES] = tile.T

    def softplus2(x):
        y = lax.log2(1.0 + lax.exp2(jnp.minimum(x, 100.0)))
        return jnp.maximum(y, x).astype(BF)

    def body(levels, nets):
        def push_shocked(q, j):
            g = (2 * (j % STEPS) + q) * 2
            both = jnp.concatenate([shocked[g], shocked[g + 1]], 1)
            pltpu.matmul_push_rhs(both, staging_register=0, mxu_index=q)

        def level(q, j, p, slot):
            side = sides[slot][p * PIECE:(p + 1) * PIECE]
            pltpu.matmul_acc_lhs(
                levels[q][j % 2][p], jnp.concatenate([side, side], 1), load_staged_rhs=0 if p == 0 else None
            )

        def net(q, j, chosen):
            values = staged[q][j % 2]
            pltpu.matmul_push_rhs(jnp.concatenate([values[0], values[1]], 1), staging_register=1, mxu_index=q)
            pltpu.matmul_acc_lhs(nets[q][j], chosen, load_staged_rhs=1)

        for q in range(2):
            for acc in nets[q]:
                pltpu.matmul_pop(acc)
            for r in range(2):
                for p in range(PIECES):
                    pltpu.matmul_pop(levels[q][r][p])
        prepare(0, 0)
        for j in range(2):
            for q in range(2):
                push_shocked(q, j)
                for p in range(PIECES):
                    level(q, j, p, 0)
        members_ref[...] = jnp.zeros_like(members_ref)
        for q in range(2):
            staged[q][1][...] = jnp.zeros_like(stage00)

        def shard(s, parity, chosen, before):
            for j in range(STEPS):
                if j == 0:
                    prepare(lax.min(s + 1, NPA - 1), 1 - parity)
                slot = parity if j + 2 < STEPS else 1 - parity
                for q in range(2):
                    push_shocked(q, j + 2)
                for p in range(PIECES):
                    for q in range(2):
                        x = pltpu.matmul_pop(levels[q][j % 2][p])
                        level(q, j + 2, p, slot)
                        value = softplus2(x)
                        for h in range(2):
                            staged[q][j % 2][h, p * PIECE:(p + 1) * PIECE] = value[:, h * LANES:(h + 1) * LANES]
                for q in range(2):
                    net(q, (j - 1) % STEPS, chosen if j else before)

        def pair_of_shards(i, carry):
            tile_copy(2 * i + 1, pa).wait_recv()

            @pl.when(i < NPA // 2 - 1)
            def _():
                tile_copy(2 * i + 2, pa).wait_recv()

            before = members_ref[...]
            for parity in range(2):
                chosen = members(2 * i + parity)
                shard(2 * i + parity, parity, chosen, before)
                before = chosen
            members_ref[...] = before
            return carry

        lax.fori_loop(0, NPA // 2, pair_of_shards, 0)
        for q in range(2):
            net(q, STEPS - 1, members_ref[...])
            for r in range(2):
                for p in range(PIECES):
                    pltpu.matmul_pop(levels[q][r][p])

        lane = lax.broadcasted_iota(jnp.int32, (SETS, LANES), 1)
        partial = jnp.zeros((SETS, LANES), F32)
        for j in range(STEPS):
            for q in range(2):
                netted = pltpu.matmul_pop(nets[q][j])
                for h in range(2):
                    g = (2 * j + q) * 2 + h
                    d = g % DATES
                    exposure = netted[:, h * LANES:(h + 1) * LANES] * (0.0625 * LN2) * discount[d:d + 1, :].astype(F32)
                    positive = jnp.sum(jnp.maximum(exposure, 0.0), axis=1, keepdims=True)
                    negative = jnp.sum(jnp.minimum(exposure, 0.0), axis=1, keepdims=True)
                    partial = jnp.where(lane == g, positive, partial)
                    partial = jnp.where(lane == GROUPS + g, negative, partial)
        sums[...] = partial

    acc = lambda q, m: pltpu.ACC(q)((m, 256), F32)
    pl.run_scoped(
        body,
        [[[acc(q, PIECE) for _ in range(PIECES)] for _ in range(2)] for q in range(2)],
        [[acc(q, SETS) for _ in range(STEPS)] for q in range(2)],
    )

    for k in range(NPA):
        info = tiles[k, 0, K:ROWS].astype(F32)
        coefs[pl.ds(shifted(pa, OFFSETS[k]), 1), :] = info[5:6, :] + info[6:7, :] + info[7:8, :]
    partial = sums[...] * (1.0 / (NPA * LANES))
    totals = jnp.sum(partial * coefs[...], axis=0, keepdims=True)
    rows = partial + pltpu.roll(jnp.broadcast_to(totals, (8, LANES)), 64, 1)[0:1, :]
    for n in range(SETS):
        outbox[n] = rows[n:n + 1, :]

    def row_copy(k, target):
        return pltpu.make_async_remote_copy(
            src_ref=outbox.at[target], dst_ref=inbox.at[k], send_sem=out_sems.at[k], recv_sem=in_sems.at[k],
            device_id={"pa": target}, device_id_type=MESH,
        )

    for k in range(NPA - 1, 0, -1):
        row_copy(k, shifted(pa, OFFSETS[k])).start()
    inbox[0] = outbox[pa]
    for k in range(1, NPA):
        row_copy(k, shifted(pa, OFFSETS[k])).wait_recv()
    mine = jnp.sum(inbox[...], axis=0)

    lane = lax.broadcasted_iota(jnp.int32, (1, LANES), 1)
    weighted = mine * coef
    first = lax.rem(lane // DATES, 2) == 0
    upper = lane >= 64

    def lane_sum(value, mask):
        return jnp.sum(jnp.where(mask, value, 0.0), axis=1, keepdims=True)

    adjust = [lane_sum(weighted, first), lane_sum(weighted, jnp.logical_not(first))]
    total = [
        lane_sum(mine, jnp.logical_and(first, upper)),
        lane_sum(mine, jnp.logical_and(jnp.logical_not(first), upper)),
    ]
    near_out[...] = jnp.broadcast_to(adjust[0] + adjust[1], (1, LANES))

    def near_copy(hop, target):
        return pltpu.make_async_remote_copy(
            src_ref=near_out, dst_ref=near_in.at[hop], send_sem=near_send.at[hop], recv_sem=near_recv.at[hop],
            device_id={"sa": target}, device_id_type=MESH,
        )

    for hop in range(1, NSA):
        near_copy(hop, lax.rem(sa + hop, NSA)).start()
    near_in[0] = near_out[...]

    for hop in range(1, NSA):
        near_copy(hop, lax.rem(sa + hop, NSA)).wait_recv()
    mean = jnp.sum(near_in[...], axis=0)[:, 0:1] / (2 * NSA)
    row = mine
    for i, value in enumerate([adjust[0] - mean, adjust[1] - mean, *total]):
        row = jnp.where(lane == 64 + i, value, row)
    result[...] = row

    for k in range(1, NPA):
        tile_copy(k, pa).wait_send()
        row_copy(k, shifted(pa, OFFSETS[k])).wait_send()
    for hop in range(1, NSA):
        near_copy(hop, sa).wait_send()


def spread(row, profile_out, xva_out, total_out):
    values = row[...]
    for sign in range(2):
        for s in range(2):
            start = sign * 32 + s * 16
            profile_out[sign, s:s + 1, :] = values[:, start:start + DATES]
    xva_out[...] = values[:, 64:66]
    total_out[...] = values[:, 66:68]


def on_device(
    factors, trade_weights, payoff_terms, set_blocks, shock_pick, shock_scale, shock_shift, discount, set_pd, own_pd
):
    vmem = pl.BlockSpec(memory_space=pltpu.VMEM)
    arrays = [
        set_blocks, shock_pick, factors, trade_weights, payoff_terms, shock_scale, shock_shift, discount, set_pd,
        own_pd.reshape(1, DATES),
    ]
    row = pl.pallas_call(
        kernel,
        out_shape=jax.ShapeDtypeStruct((1, LANES), F32),
        in_specs=[pl.BlockSpec(memory_space=pl.ANY)] * 10,
        out_specs=vmem,
        scratch_shapes=[
            *(pltpu.SMEM(a.shape, a.dtype) for a in arrays[:2]),
            *(pltpu.VMEM(a.shape, a.dtype) for a in arrays[2:]),
            pltpu.VMEM((NPA, 2, ROWS, LANES), BF),
            pltpu.VMEM((GROUPS, 256, LANES), BF),
            pltpu.VMEM((K * DATES, LANES), F32),
            *(pltpu.VMEM((256, LANES), BF) for _ in range(2)),
            *(pltpu.VMEM((2, 256, LANES), BF) for _ in range(4)),
            pltpu.VMEM((SETS, 256), BF),
            pltpu.VMEM((8, LANES), F32),
            pltpu.VMEM((SETS, LANES), F32),
            pltpu.VMEM((SETS, LANES), F32),
            pltpu.VMEM((SETS, 1, LANES), F32),
            pltpu.VMEM((NPA, 1, LANES), F32),
            pltpu.VMEM((1, LANES), F32),
            pltpu.VMEM((NSA, 1, LANES), F32),
            pltpu.SemaphoreType.DMA((10,)),
            pltpu.SemaphoreType.DMA((NPA,)),
            pltpu.SemaphoreType.DMA((NPA,)),
            pltpu.SemaphoreType.DMA((NPA,)),
            pltpu.SemaphoreType.DMA((NPA,)),
            pltpu.SemaphoreType.DMA((NSA,)),
            pltpu.SemaphoreType.DMA((NSA,)),
        ],
        compiler_params=pltpu.CompilerParams(
            collective_id=0, has_side_effects=True, vmem_limit_bytes=60 << 20
        ),
        name="valuation",
    )(*arrays)
    profile, xva, total = pl.pallas_call(
        spread,
        out_shape=(
            jax.ShapeDtypeStruct((2, 2, DATES), F32),
            jax.ShapeDtypeStruct((1, 2), F32),
            jax.ShapeDtypeStruct((1, 2), F32),
        ),
        in_specs=[vmem],
        out_specs=(vmem, vmem, vmem),
        name="spread",
    )(row)
    return profile.transpose(0, 2, 1).reshape(2, 1, DATES, 2), xva, total.reshape(2)


def solution(mesh):
    return jax.shard_map(
        on_device,
        mesh=mesh,
        in_specs=(
            P(None, None, "pa"), P(None, "pa"), P(None, "pa"), P(), P("sa"), P(), P(), P(None, "pa"),
            P("pa", None), P(),
        ),
        out_specs=(P(None, "pa", None, "sa"), P("pa", "sa"), P("sa")),
        check_vma=False,
    )
```

```python
import functools

import jax
import jax.numpy as jnp
from jax import lax
from jax.experimental import pallas as pl
from jax.experimental.pallas import tpu as pltpu
from jax.sharding import PartitionSpec as P

BF = jnp.bfloat16
F32 = jnp.float32
K = 64
SETS = 32
DATES = 16
LANES = 128
ROWS = 80
GROUPS = 32
STEPS = 8
PIECE = 128
PIECES = 2
NZ, NX, NPA, NSA = 8, 4, 32, 8
LOG2E = 1.4426950408889634
LN2 = 0.6931471805599453
MESH = pl.DeviceIdType.MESH
FIRST, LAST, AHEAD = 4, 14, 2
BOTH = range(1, 2 * FIRST + 1)


def ring(delta, extent):
    return min(delta, extent - delta)


OFFSETS = sorted(
    ((dz, dx) for dz in range(NZ) for dx in range(NX)),
    key=lambda o: (ring(o[0], NZ) + ring(o[1], NX), ring(o[0], NZ), o[0] > NZ // 2, o[1]),
)


def shifted(me, offset):
    z, x = me // NX, lax.rem(me, NX)
    return lax.rem(z + offset[0], NZ) * NX + lax.rem(x + offset[1], NX)


def back(offset):
    return ((NZ - offset[0]) % NZ, (NX - offset[1]) % NX)


def parts_of(value):
    high = value.astype(BF).astype(F32)
    rest = value - high
    middle = rest.astype(BF).astype(F32)
    return high, middle, rest - middle


def kernel(
    *refs,
):
    hbm, refs = refs[:10], refs[10:]
    result, refs = refs[0], refs[1:]
    local, refs = refs[:10], refs[10:]
    blocks, pick, factors, weights, terms, scale, shift, discount, set_pd, own_pd = local
    (
        tiles, shocked, flat, side0, side1, stage00, stage01, stage10, stage11, members_ref, coef_row, coefs, sums,
        outbox, inbox, near_out, near_in,
        load_sems, send_sems, tile_sems, relay_sems, out_sems, in_sems, near_send, near_recv,
    ) = refs
    core = lax.rem(lax.axis_index("sa"), 2)
    sides = [side0, side1]
    staged = [[stage00, stage01], [stage10, stage11]]
    pa = lax.axis_index("pa")
    sa = lax.axis_index("sa")
    loads = [pltpu.make_async_copy(hbm[i], local[i], load_sems.at[i]) for i in range(10)]
    for load in loads:
        load.start()

    barrier = pltpu.get_barrier_semaphore()
    for offset in OFFSETS[1:]:
        pl.semaphore_signal(barrier, inc=1, device_id={"pa": shifted(pa, offset)}, device_id_type=MESH)
    for hop in range(1, NSA):
        pl.semaphore_signal(barrier, inc=1, device_id={"sa": lax.rem(sa + hop, NSA)}, device_id_type=MESH)

    for i in (0, 3, 4, 8, 9):
        loads[i].wait()

    coef_row[...] = jnp.zeros_like(coef_row)
    coef_row[0:1, 0:16] = set_pd[...]
    coef_row[0:1, 16:32] = set_pd[...]
    coef_row[0:1, 32:48] = own_pd[...]
    coef_row[0:1, 48:64] = own_pd[...]
    coef = coef_row[0:1, :]
    ends = []
    running = jnp.int32(0)
    for m in range(SETS):
        running = running + blocks[m]
        ends.append(running)
    row = lax.broadcasted_iota(jnp.int32, (16, LANES), 0)
    for half in range(2):
        block = 2 * pa + half
        owner = jnp.int32(0)
        for end in ends:
            owner = owner + jnp.where(end <= block, 1, 0).astype(jnp.int32)
        lanes = slice(half * LANES, (half + 1) * LANES)
        notional = terms[0:1, lanes].astype(F32)
        strike = parts_of(terms[1:2, lanes].astype(F32) * LOG2E)
        rows = [*strike, notional, jnp.full((1, LANES), owner.astype(F32))]
        if half == 0:
            rows.extend(parts_of(coef))
        block_rows = jnp.zeros((16, LANES), F32)
        for i, value in enumerate(rows):
            block_rows = jnp.where(row == i, value, block_rows)
        tiles[0, half, 0:K] = weights[:, lanes]
        tiles[0, half, K:ROWS] = block_rows.astype(BF)

    for i in (1, 2, 5, 6, 7):
        loads[i].wait()
    for k in range(K):
        flat[k * DATES:(k + 1) * DATES, :] = factors[k].astype(F32)
    ones = jnp.where(lax.broadcasted_iota(jnp.int32, (K, LANES), 0) < 3, 1.0, 0.0).astype(BF)
    none = jnp.zeros((K, LANES), BF)
    for s in range(2):
        which = pick[s]
        scales = jnp.broadcast_to(scale[pl.ds(which, 1), :], (LANES, K)).T
        shifts = jnp.broadcast_to(shift[pl.ds(which, 1), :], (LANES, K)).T
        for d in range(DATES):
            g = s * DATES + d
            base = flat[pl.ds(d, K, stride=DATES), :]
            value = (scales * base + shifts).astype(BF).astype(F32) * LOG2E
            high = value.astype(BF)
            shocked[g, 0:K] = high
            shocked[g, K:2 * K] = ones
            shocked[g, 2 * K:3 * K] = (value - high.astype(F32)).astype(BF)
            shocked[g, 3 * K:4 * K] = none

    pl.semaphore_wait(barrier, NPA - 1 + NSA - 1)

    def tile_copy(k, target):
        return pltpu.make_async_remote_copy(
            src_ref=tiles.at[0], dst_ref=tiles.at[k], send_sem=send_sems.at[k], recv_sem=tile_sems.at[k],
            device_id={"pa": target}, device_id_type=MESH,
        )

    def relay(k):
        return pltpu.make_async_remote_copy(
            src_ref=tiles.at[k], dst_ref=tiles.at[k], send_sem=relay_sems.at[k], recv_sem=tile_sems.at[k],
            device_id={"sa": sa + 1 - 2 * core}, device_id_type=MESH,
        )

    def half_of(k):
        targets = [shifted(pa, back(OFFSETS[k + c])) for c in range(2)]
        return tile_copy(k + core, jnp.where(core == 0, targets[0], targets[1]))

    for k in BOTH:
        tile_copy(k, shifted(pa, back(OFFSETS[k]))).start()
    for i in range(FIRST, LAST + 1):
        half_of(2 * i + 1).start()
    tile_copy(NPA - 1, shifted(pa, back(OFFSETS[NPA - 1]))).start()

    def members(s):
        halves = []
        for half in range(2):
            info = tiles[s, half, K:ROWS].astype(F32)
            ids = lax.broadcasted_iota(jnp.int32, (SETS, LANES), 0).astype(F32)
            halves.append(jnp.where(ids == info[4:5, :], info[3:4, :], 0.0).astype(BF))
        return jnp.concatenate(halves, 1)

    def prepare(s, slot):
        for half in range(2):
            tile = jnp.concatenate([tiles[s, half], jnp.zeros((LANES - ROWS, LANES), BF)], 0)
            sides[slot][half * LANES:(half + 1) * LANES] = tile.T

    def softplus2(x):
        y = lax.log2(1.0 + lax.exp2(jnp.minimum(x, 100.0)))
        return jnp.maximum(y, x).astype(BF)

    def body(levels, nets):
        def push_shocked(q, j):
            g = (2 * (j % STEPS) + q) * 2
            both = jnp.concatenate([shocked[g], shocked[g + 1]], 1)
            pltpu.matmul_push_rhs(both, staging_register=0, mxu_index=q)

        def level(q, j, p, slot):
            side = sides[slot][p * PIECE:(p + 1) * PIECE]
            pltpu.matmul_acc_lhs(
                levels[q][j % 2][p], jnp.concatenate([side, side], 1), load_staged_rhs=0 if p == 0 else None
            )

        def net(q, j, chosen):
            values = staged[q][j % 2]
            pltpu.matmul_push_rhs(jnp.concatenate([values[0], values[1]], 1), staging_register=1, mxu_index=q)
            pltpu.matmul_acc_lhs(nets[q][j], chosen, load_staged_rhs=1)

        for q in range(2):
            for acc in nets[q]:
                pltpu.matmul_pop(acc)
            for r in range(2):
                for p in range(PIECES):
                    pltpu.matmul_pop(levels[q][r][p])
        prepare(0, 0)
        for j in range(2):
            for q in range(2):
                push_shocked(q, j)
                for p in range(PIECES):
                    level(q, j, p, 0)
        members_ref[...] = jnp.zeros_like(members_ref)
        for q in range(2):
            staged[q][1][...] = jnp.zeros_like(stage00)

        def shard(s, parity, chosen, before):
            for j in range(STEPS):
                if j == 0:
                    prepare(lax.min(s + 1, NPA - 1), 1 - parity)
                slot = parity if j + 2 < STEPS else 1 - parity
                for q in range(2):
                    push_shocked(q, j + 2)
                for p in range(PIECES):
                    for q in range(2):
                        x = pltpu.matmul_pop(levels[q][j % 2][p])
                        level(q, j + 2, p, slot)
                        value = softplus2(x)
                        for h in range(2):
                            staged[q][j % 2][h, p * PIECE:(p + 1) * PIECE] = value[:, h * LANES:(h + 1) * LANES]
                for q in range(2):
                    net(q, (j - 1) % STEPS, chosen if j else before)

        def pair_of_shards(i, carry):
            @pl.when(i < FIRST)
            def _():
                tile_copy(2 * i + 1, pa).wait_recv()
                tile_copy(2 * i + 2, pa).wait_recv()

            @pl.when(jnp.logical_and(i >= FIRST - AHEAD, i <= LAST - AHEAD))
            def _():
                k = 2 * (i + AHEAD) + 1 + core
                tile_copy(k, pa).wait_recv()
                relay(k).start()

            @pl.when(jnp.logical_and(i >= FIRST, i <= LAST))
            def _():
                tile_copy(2 * i + 2 - core, pa).wait_recv()

            @pl.when(i > LAST)
            def _():
                tile_copy(NPA - 1, pa).wait_recv()

            before = members_ref[...]
            for parity in range(2):
                chosen = members(2 * i + parity)
                shard(2 * i + parity, parity, chosen, before)
                before = chosen
            members_ref[...] = before
            return carry

        lax.fori_loop(0, NPA // 2, pair_of_shards, 0)
        for q in range(2):
            net(q, STEPS - 1, members_ref[...])
            for r in range(2):
                for p in range(PIECES):
                    pltpu.matmul_pop(levels[q][r][p])

        lane = lax.broadcasted_iota(jnp.int32, (SETS, LANES), 1)
        partial = jnp.zeros((SETS, LANES), F32)
        for j in range(STEPS):
            for q in range(2):
                netted = pltpu.matmul_pop(nets[q][j])
                for h in range(2):
                    g = (2 * j + q) * 2 + h
                    d = g % DATES
                    exposure = netted[:, h * LANES:(h + 1) * LANES] * (0.0625 * LN2) * discount[d:d + 1, :].astype(F32)
                    positive = jnp.sum(jnp.maximum(exposure, 0.0), axis=1, keepdims=True)
                    negative = jnp.sum(jnp.minimum(exposure, 0.0), axis=1, keepdims=True)
                    partial = jnp.where(lane == g, positive, partial)
                    partial = jnp.where(lane == GROUPS + g, negative, partial)
        sums[...] = partial

    acc = lambda q, m: pltpu.ACC(q)((m, 256), F32)
    pl.run_scoped(
        body,
        [[[acc(q, PIECE) for _ in range(PIECES)] for _ in range(2)] for q in range(2)],
        [[acc(q, SETS) for _ in range(STEPS)] for q in range(2)],
    )

    for k in range(NPA):
        info = tiles[k, 0, K:ROWS].astype(F32)
        coefs[pl.ds(shifted(pa, OFFSETS[k]), 1), :] = info[5:6, :] + info[6:7, :] + info[7:8, :]
    partial = sums[...] * (1.0 / (NPA * LANES))
    totals = jnp.sum(partial * coefs[...], axis=0, keepdims=True)
    rows = partial + pltpu.roll(jnp.broadcast_to(totals, (8, LANES)), 64, 1)[0:1, :]
    for n in range(SETS):
        outbox[n] = rows[n:n + 1, :]

    def row_copy(k, target):
        return pltpu.make_async_remote_copy(
            src_ref=outbox.at[target], dst_ref=inbox.at[k], send_sem=out_sems.at[k], recv_sem=in_sems.at[k],
            device_id={"pa": target}, device_id_type=MESH,
        )

    for k in range(NPA - 1, 0, -1):
        row_copy(k, shifted(pa, OFFSETS[k])).start()
    inbox[0] = outbox[pa]
    for k in range(1, NPA):
        row_copy(k, shifted(pa, OFFSETS[k])).wait_recv()
    mine = jnp.sum(inbox[...], axis=0)

    lane = lax.broadcasted_iota(jnp.int32, (1, LANES), 1)
    weighted = mine * coef
    first = lax.rem(lane // DATES, 2) == 0
    upper = lane >= 64

    def lane_sum(value, mask):
        return jnp.sum(jnp.where(mask, value, 0.0), axis=1, keepdims=True)

    adjust = [lane_sum(weighted, first), lane_sum(weighted, jnp.logical_not(first))]
    total = [
        lane_sum(mine, jnp.logical_and(first, upper)),
        lane_sum(mine, jnp.logical_and(jnp.logical_not(first), upper)),
    ]
    near_out[...] = jnp.broadcast_to(adjust[0] + adjust[1], (1, LANES))

    def near_copy(hop, target):
        return pltpu.make_async_remote_copy(
            src_ref=near_out, dst_ref=near_in.at[hop], send_sem=near_send.at[hop], recv_sem=near_recv.at[hop],
            device_id={"sa": target}, device_id_type=MESH,
        )

    for hop in range(1, NSA):
        near_copy(hop, lax.rem(sa + hop, NSA)).start()
    near_in[0] = near_out[...]

    for hop in range(1, NSA):
        near_copy(hop, lax.rem(sa + hop, NSA)).wait_recv()
    mean = jnp.sum(near_in[...], axis=0)[:, 0:1] / (2 * NSA)
    row = mine
    for i, value in enumerate([adjust[0] - mean, adjust[1] - mean, *total]):
        row = jnp.where(lane == 64 + i, value, row)
    result[...] = row

    for k in (*BOTH, NPA - 1):
        tile_copy(k, pa).wait_send()
    for i in range(FIRST, LAST + 1):
        half_of(2 * i + 1).wait_send()
        relay(2 * i + 1 + core).wait_send()
    for k in range(1, NPA):
        row_copy(k, shifted(pa, OFFSETS[k])).wait_send()
    for hop in range(1, NSA):
        near_copy(hop, sa).wait_send()


def spread(row, profile_out, xva_out, total_out):
    values = row[...]
    for sign in range(2):
        for s in range(2):
            start = sign * 32 + s * 16
            profile_out[sign, s:s + 1, :] = values[:, start:start + DATES]
    xva_out[...] = values[:, 64:66]
    total_out[...] = values[:, 66:68]


def on_device(
    factors, trade_weights, payoff_terms, set_blocks, shock_pick, shock_scale, shock_shift, discount, set_pd, own_pd
):
    vmem = pl.BlockSpec(memory_space=pltpu.VMEM)
    arrays = [
        set_blocks, shock_pick, factors, trade_weights, payoff_terms, shock_scale, shock_shift, discount, set_pd,
        own_pd.reshape(1, DATES),
    ]
    row = pl.pallas_call(
        kernel,
        out_shape=jax.ShapeDtypeStruct((1, LANES), F32),
        in_specs=[pl.BlockSpec(memory_space=pl.ANY)] * 10,
        out_specs=vmem,
        scratch_shapes=[
            *(pltpu.SMEM(a.shape, a.dtype) for a in arrays[:2]),
            *(pltpu.VMEM(a.shape, a.dtype) for a in arrays[2:]),
            pltpu.VMEM((NPA, 2, ROWS, LANES), BF),
            pltpu.VMEM((GROUPS, 256, LANES), BF),
            pltpu.VMEM((K * DATES, LANES), F32),
            *(pltpu.VMEM((256, LANES), BF) for _ in range(2)),
            *(pltpu.VMEM((2, 256, LANES), BF) for _ in range(4)),
            pltpu.VMEM((SETS, 256), BF),
            pltpu.VMEM((8, LANES), F32),
            pltpu.VMEM((SETS, LANES), F32),
            pltpu.VMEM((SETS, LANES), F32),
            pltpu.VMEM((SETS, 1, LANES), F32),
            pltpu.VMEM((NPA, 1, LANES), F32),
            pltpu.VMEM((1, LANES), F32),
            pltpu.VMEM((NSA, 1, LANES), F32),
            pltpu.SemaphoreType.DMA((10,)),
            pltpu.SemaphoreType.DMA((NPA,)),
            pltpu.SemaphoreType.DMA((NPA,)),
            pltpu.SemaphoreType.DMA((NPA,)),
            pltpu.SemaphoreType.DMA((NPA,)),
            pltpu.SemaphoreType.DMA((NPA,)),
            pltpu.SemaphoreType.DMA((NSA,)),
            pltpu.SemaphoreType.DMA((NSA,)),
        ],
        compiler_params=pltpu.CompilerParams(
            collective_id=0, has_side_effects=True, vmem_limit_bytes=60 << 20
        ),
        name="valuation",
    )(*arrays)
    profile, xva, total = pl.pallas_call(
        spread,
        out_shape=(
            jax.ShapeDtypeStruct((2, 2, DATES), F32),
            jax.ShapeDtypeStruct((1, 2), F32),
            jax.ShapeDtypeStruct((1, 2), F32),
        ),
        in_specs=[vmem],
        out_specs=(vmem, vmem, vmem),
        name="spread",
    )(row)
    return profile.transpose(0, 2, 1).reshape(2, 1, DATES, 2), xva, total.reshape(2)


def solution(mesh):
    return jax.shard_map(
        on_device,
        mesh=mesh,
        in_specs=(
            P(None, None, "pa"), P(None, "pa"), P(None, "pa"), P(), P("sa"), P(), P(), P(None, "pa"),
            P("pa", None), P(),
        ),
        out_specs=(P(None, "pa", None, "sa"), P("pa", "sa"), P("sa")),
        check_vma=False,
    )
```

```python
import functools

import jax
import jax.numpy as jnp
from jax import lax
from jax.experimental import pallas as pl
from jax.experimental.pallas import tpu as pltpu
from jax.sharding import PartitionSpec as P

BF = jnp.bfloat16
F32 = jnp.float32
K = 64
SETS = 32
DATES = 16
LANES = 128
ROWS = 80
GROUPS = 32
STEPS = 8
PIECE = 128
PIECES = 2
NZ, NX, NPA, NSA = 8, 4, 32, 8
LOG2E = 1.4426950408889634
LN2 = 0.6931471805599453
MESH = pl.DeviceIdType.MESH


OFFSETS = [(dz, dx) for dz in (0, 1, 7, 2, 6, 3, 5, 4) for dx in (0, 1, 3, 2)]
NEAR = (1, 2, 3, 4, 8)


def shifted(me, offset):
    z, x = me // NX, lax.rem(me, NX)
    return lax.rem(z + offset[0], NZ) * NX + lax.rem(x + offset[1], NX)


def back(offset):
    return ((NZ - offset[0]) % NZ, (NX - offset[1]) % NX)


def parts_of(value):
    high = value.astype(BF).astype(F32)
    rest = value - high
    middle = rest.astype(BF).astype(F32)
    return high, middle, rest - middle


def kernel(
    *refs,
):
    hbm, refs = refs[:10], refs[10:]
    result, refs = refs[0], refs[1:]
    local, refs = refs[:10], refs[10:]
    blocks, pick, factors, weights, terms, scale, shift, discount, set_pd, own_pd = local
    (
        tiles, shocked, flat, side0, side1, stage00, stage01, stage10, stage11, members_ref, coef_row, coefs, sums,
        outbox, inbox, near_out, near_in,
        load_sems, send_sems, tile_sems, out_sems, in_sems, near_send, near_recv,
    ) = refs
    sides = [side0, side1]
    staged = [[stage00, stage01], [stage10, stage11]]
    pa = lax.axis_index("pa")
    sa = lax.axis_index("sa")
    loads = [pltpu.make_async_copy(hbm[i], local[i], load_sems.at[i]) for i in range(10)]
    for load in loads:
        load.start()

    barrier = pltpu.get_barrier_semaphore()
    for k in NEAR:
        pl.semaphore_signal(barrier, inc=1, device_id={"pa": shifted(pa, OFFSETS[k])}, device_id_type=MESH)
    for hop in range(1, NSA):
        pl.semaphore_signal(barrier, inc=1, device_id={"sa": lax.rem(sa + hop, NSA)}, device_id_type=MESH)

    for i in (0, 3, 4, 8, 9):
        loads[i].wait()

    coef_row[...] = jnp.zeros_like(coef_row)
    coef_row[0:1, 0:16] = set_pd[...]
    coef_row[0:1, 16:32] = set_pd[...]
    coef_row[0:1, 32:48] = own_pd[...]
    coef_row[0:1, 48:64] = own_pd[...]
    coef = coef_row[0:1, :]
    ends = []
    running = jnp.int32(0)
    for m in range(SETS):
        running = running + blocks[m]
        ends.append(running)
    row = lax.broadcasted_iota(jnp.int32, (16, LANES), 0)
    for half in range(2):
        block = 2 * pa + half
        owner = jnp.int32(0)
        for end in ends:
            owner = owner + jnp.where(end <= block, 1, 0).astype(jnp.int32)
        lanes = slice(half * LANES, (half + 1) * LANES)
        notional = terms[0:1, lanes].astype(F32)
        strike = parts_of(terms[1:2, lanes].astype(F32) * LOG2E)
        rows = [*strike, notional, jnp.full((1, LANES), owner.astype(F32))]
        if half == 0:
            rows.extend(parts_of(coef))
        block_rows = jnp.zeros((16, LANES), F32)
        for i, value in enumerate(rows):
            block_rows = jnp.where(row == i, value, block_rows)
        tiles[0, half, 0:K] = weights[:, lanes]
        tiles[0, half, K:ROWS] = block_rows.astype(BF)

    for i in (1, 2, 5, 6, 7):
        loads[i].wait()
    for k in range(K):
        flat[k * DATES:(k + 1) * DATES, :] = factors[k].astype(F32)
    ones = jnp.where(lax.broadcasted_iota(jnp.int32, (K, LANES), 0) < 3, 1.0, 0.0).astype(BF)
    none = jnp.zeros((K, LANES), BF)
    for s in range(2):
        which = pick[s]
        scales = jnp.broadcast_to(scale[pl.ds(which, 1), :], (LANES, K)).T
        shifts = jnp.broadcast_to(shift[pl.ds(which, 1), :], (LANES, K)).T
        for d in range(DATES):
            g = s * DATES + d
            base = flat[pl.ds(d, K, stride=DATES), :]
            value = (scales * base + shifts).astype(BF).astype(F32) * LOG2E
            high = value.astype(BF)
            shocked[g, 0:K] = high
            shocked[g, K:2 * K] = ones
            shocked[g, 2 * K:3 * K] = (value - high.astype(F32)).astype(BF)
            shocked[g, 3 * K:4 * K] = none

    pl.semaphore_wait(barrier, len(NEAR) + NSA - 1)

    def tile_copy(source, k, target):
        return pltpu.make_async_remote_copy(
            src_ref=tiles.at[source], dst_ref=tiles.at[k], send_sem=send_sems.at[k], recv_sem=tile_sems.at[k],
            device_id={"pa": target}, device_id_type=MESH,
        )

    def arrived(k):
        tile_copy(k, k, pa).wait_recv()

    def pass_on(source, k):
        odd = lax.rem(k // NX, 2)
        target = lax.rem(pa // NX + 1 + (NZ - 2) * odd, NZ) * NX + lax.rem(pa, NX)
        tile_copy(source, k, target).start()

    for k in NEAR:
        tile_copy(0, k, shifted(pa, back(OFFSETS[k]))).start()

    def members(s):
        halves = []
        for half in range(2):
            info = tiles[s, half, K:ROWS].astype(F32)
            ids = lax.broadcasted_iota(jnp.int32, (SETS, LANES), 0).astype(F32)
            halves.append(jnp.where(ids == info[4:5, :], info[3:4, :], 0.0).astype(BF))
        return jnp.concatenate(halves, 1)

    def prepare(s, slot):
        for half in range(2):
            tile = jnp.concatenate([tiles[s, half], jnp.zeros((LANES - ROWS, LANES), BF)], 0)
            sides[slot][half * LANES:(half + 1) * LANES] = tile.T

    def softplus2(x):
        y = lax.log2(1.0 + lax.exp2(jnp.minimum(x, 100.0)))
        return jnp.maximum(y, x).astype(BF)

    def body(levels, nets):
        def push_shocked(q, j):
            g = (2 * (j % STEPS) + q) * 2
            both = jnp.concatenate([shocked[g], shocked[g + 1]], 1)
            pltpu.matmul_push_rhs(both, staging_register=0, mxu_index=q)

        def level(q, j, p, slot):
            side = sides[slot][p * PIECE:(p + 1) * PIECE]
            pltpu.matmul_acc_lhs(
                levels[q][j % 2][p], jnp.concatenate([side, side], 1), load_staged_rhs=0 if p == 0 else None
            )

        def net(q, j, chosen):
            values = staged[q][j % 2]
            pltpu.matmul_push_rhs(jnp.concatenate([values[0], values[1]], 1), staging_register=1, mxu_index=q)
            pltpu.matmul_acc_lhs(nets[q][j], chosen, load_staged_rhs=1)

        for q in range(2):
            for acc in nets[q]:
                pltpu.matmul_pop(acc)
            for r in range(2):
                for p in range(PIECES):
                    pltpu.matmul_pop(levels[q][r][p])
        prepare(0, 0)
        for j in range(2):
            for q in range(2):
                push_shocked(q, j)
                for p in range(PIECES):
                    level(q, j, p, 0)

        def shard(s, parity, chosen, before, first=False, last=False):
            for j in range(STEPS):
                if first and j == 4:
                    arrived(1)
                    pass_on(1, 5)
                    pass_on(1, 9)
                if not last and j == (4 if first else 0):
                    prepare(s + 1, 1 - parity)
                slot = parity if j + 2 < STEPS else 1 - parity
                ahead = not last or j + 2 < STEPS
                if ahead:
                    for q in range(2):
                        push_shocked(q, j + 2)
                for p in range(PIECES):
                    for q in range(2):
                        x = pltpu.matmul_pop(levels[q][j % 2][p])
                        if ahead:
                            level(q, j + 2, p, slot)
                        value = softplus2(x)
                        for h in range(2):
                            staged[q][j % 2][h, p * PIECE:(p + 1) * PIECE] = value[:, h * LANES:(h + 1) * LANES]
                if j or not first:
                    for q in range(2):
                        net(q, (j - 1) % STEPS, chosen if j else before)

        chosen = members(0)
        shard(0, 0, chosen, None, first=True)
        members_ref[...] = chosen

        def pair_of_shards(i, carry):
            arrived(2 * i + 2)
            arrived(2 * i + 3)

            @pl.when(i == 0)
            def _():
                for k in (2, 3):
                    pass_on(k, k + 4)
                    pass_on(k, k + 8)

            @pl.when(jnp.logical_and(i >= 1, i <= 10))
            def _():
                for k in (2 * i + 2, 2 * i + 3):
                    pass_on(k, k + 8)

            before = members_ref[...]
            for parity in (1, 0):
                s = 2 * i + 2 - parity
                chosen = members(s)
                shard(s, parity, chosen, before)
                before = chosen
            members_ref[...] = before
            return carry

        lax.fori_loop(0, NPA // 2 - 1, pair_of_shards, 0)
        chosen = members(NPA - 1)
        shard(NPA - 1, 1, chosen, members_ref[...], last=True)
        for q in range(2):
            net(q, STEPS - 1, chosen)

        lane = lax.broadcasted_iota(jnp.int32, (SETS, LANES), 1)
        partial = jnp.zeros((SETS, LANES), F32)
        for j in range(STEPS):
            for q in range(2):
                netted = pltpu.matmul_pop(nets[q][j])
                for h in range(2):
                    g = (2 * j + q) * 2 + h
                    d = g % DATES
                    exposure = netted[:, h * LANES:(h + 1) * LANES] * (0.0625 * LN2) * discount[d:d + 1, :].astype(F32)
                    positive = jnp.sum(jnp.maximum(exposure, 0.0), axis=1, keepdims=True)
                    negative = jnp.sum(jnp.minimum(exposure, 0.0), axis=1, keepdims=True)
                    partial = jnp.where(lane == g, positive, partial)
                    partial = jnp.where(lane == GROUPS + g, negative, partial)
        sums[...] = partial

    acc = lambda q, m: pltpu.ACC(q)((m, 256), F32)
    pl.run_scoped(
        body,
        [[[acc(q, PIECE) for _ in range(PIECES)] for _ in range(2)] for q in range(2)],
        [[acc(q, SETS) for _ in range(STEPS)] for q in range(2)],
    )

    for k in range(NPA):
        info = tiles[k, 0, K:ROWS].astype(F32)
        coefs[pl.ds(shifted(pa, OFFSETS[k]), 1), :] = info[5:6, :] + info[6:7, :] + info[7:8, :]
    partial = sums[...] * (1.0 / (NPA * LANES))
    totals = jnp.sum(partial * coefs[...], axis=0, keepdims=True)
    rows = partial + pltpu.roll(jnp.broadcast_to(totals, (8, LANES)), 64, 1)[0:1, :]
    for n in range(SETS):
        outbox[n] = rows[n:n + 1, :]

    def row_copy(k, target):
        return pltpu.make_async_remote_copy(
            src_ref=outbox.at[target], dst_ref=inbox.at[k], send_sem=out_sems.at[k], recv_sem=in_sems.at[k],
            device_id={"pa": target}, device_id_type=MESH,
        )

    for k in range(NPA - 1, 0, -1):
        row_copy(k, shifted(pa, OFFSETS[k])).start()
    inbox[0] = outbox[pa]
    for k in range(1, NPA):
        row_copy(k, shifted(pa, OFFSETS[k])).wait_recv()
    mine = jnp.sum(inbox[...], axis=0)

    lane = lax.broadcasted_iota(jnp.int32, (1, LANES), 1)
    weighted = mine * coef
    first = lax.rem(lane // DATES, 2) == 0
    upper = lane >= 64

    def lane_sum(value, mask):
        return jnp.sum(jnp.where(mask, value, 0.0), axis=1, keepdims=True)

    adjust = [lane_sum(weighted, first), lane_sum(weighted, jnp.logical_not(first))]
    total = [
        lane_sum(mine, jnp.logical_and(first, upper)),
        lane_sum(mine, jnp.logical_and(jnp.logical_not(first), upper)),
    ]
    near_out[...] = jnp.broadcast_to(adjust[0] + adjust[1], (1, LANES))

    def near_copy(hop, target):
        return pltpu.make_async_remote_copy(
            src_ref=near_out, dst_ref=near_in.at[hop], send_sem=near_send.at[hop], recv_sem=near_recv.at[hop],
            device_id={"sa": target}, device_id_type=MESH,
        )

    for hop in range(1, NSA):
        near_copy(hop, lax.rem(sa + hop, NSA)).start()
    near_in[0] = near_out[...]

    for hop in range(1, NSA):
        near_copy(hop, lax.rem(sa + hop, NSA)).wait_recv()
    mean = jnp.sum(near_in[...], axis=0)[:, 0:1] / (2 * NSA)
    row = mine
    for i, value in enumerate([adjust[0] - mean, adjust[1] - mean, *total]):
        row = jnp.where(lane == 64 + i, value, row)
    result[...] = row

    for k in range(1, NPA):
        tile_copy(0, k, pa).wait_send()
        row_copy(k, shifted(pa, OFFSETS[k])).wait_send()
    for hop in range(1, NSA):
        near_copy(hop, sa).wait_send()


def spread(row, profile_out, xva_out, total_out):
    values = row[...]
    for sign in range(2):
        for s in range(2):
            start = sign * 32 + s * 16
            profile_out[sign, s:s + 1, :] = values[:, start:start + DATES]
    xva_out[...] = values[:, 64:66]
    total_out[...] = values[:, 66:68]


def on_device(
    factors, trade_weights, payoff_terms, set_blocks, shock_pick, shock_scale, shock_shift, discount, set_pd, own_pd
):
    vmem = pl.BlockSpec(memory_space=pltpu.VMEM)
    arrays = [
        set_blocks, shock_pick, factors, trade_weights, payoff_terms, shock_scale, shock_shift, discount, set_pd,
        own_pd.reshape(1, DATES),
    ]
    row = pl.pallas_call(
        kernel,
        out_shape=jax.ShapeDtypeStruct((1, LANES), F32),
        in_specs=[pl.BlockSpec(memory_space=pl.ANY)] * 10,
        out_specs=vmem,
        scratch_shapes=[
            *(pltpu.SMEM(a.shape, a.dtype) for a in arrays[:2]),
            *(pltpu.VMEM(a.shape, a.dtype) for a in arrays[2:]),
            pltpu.VMEM((NPA, 2, ROWS, LANES), BF),
            pltpu.VMEM((GROUPS, 256, LANES), BF),
            pltpu.VMEM((K * DATES, LANES), F32),
            *(pltpu.VMEM((256, LANES), BF) for _ in range(2)),
            *(pltpu.VMEM((2, 256, LANES), BF) for _ in range(4)),
            pltpu.VMEM((SETS, 256), BF),
            pltpu.VMEM((8, LANES), F32),
            pltpu.VMEM((SETS, LANES), F32),
            pltpu.VMEM((SETS, LANES), F32),
            pltpu.VMEM((SETS, 1, LANES), F32),
            pltpu.VMEM((NPA, 1, LANES), F32),
            pltpu.VMEM((1, LANES), F32),
            pltpu.VMEM((NSA, 1, LANES), F32),
            pltpu.SemaphoreType.DMA((10,)),
            pltpu.SemaphoreType.DMA((NPA,)),
            pltpu.SemaphoreType.DMA((NPA,)),
            pltpu.SemaphoreType.DMA((NPA,)),
            pltpu.SemaphoreType.DMA((NPA,)),
            pltpu.SemaphoreType.DMA((NSA,)),
            pltpu.SemaphoreType.DMA((NSA,)),
        ],
        compiler_params=pltpu.CompilerParams(
            collective_id=0, has_side_effects=True, vmem_limit_bytes=60 << 20
        ),
        name="valuation",
    )(*arrays)
    profile, xva, total = pl.pallas_call(
        spread,
        out_shape=(
            jax.ShapeDtypeStruct((2, 2, DATES), F32),
            jax.ShapeDtypeStruct((1, 2), F32),
            jax.ShapeDtypeStruct((1, 2), F32),
        ),
        in_specs=[vmem],
        out_specs=(vmem, vmem, vmem),
        name="spread",
    )(row)
    return profile.transpose(0, 2, 1).reshape(2, 1, DATES, 2), xva, total.reshape(2)


def solution(mesh):
    return jax.shard_map(
        on_device,
        mesh=mesh,
        in_specs=(
            P(None, None, "pa"), P(None, "pa"), P(None, "pa"), P(), P("sa"), P(), P(), P(None, "pa"),
            P("pa", None), P(),
        ),
        out_specs=(P(None, "pa", None, "sa"), P("pa", "sa"), P("sa")),
        check_vma=False,
    )
```

```python
import functools

import jax
import jax.numpy as jnp
from jax import lax
from jax.experimental import pallas as pl
from jax.experimental.pallas import tpu as pltpu
from jax.sharding import PartitionSpec as P

BF = jnp.bfloat16
F32 = jnp.float32
K = 64
SETS = 32
DATES = 16
LANES = 128
ROWS = 80
GROUPS = 32
STEPS = 8
PIECE = 128
PIECES = 2
NZ, NX, NPA, NSA = 8, 4, 32, 8
LOG2E = 1.4426950408889634
LN2 = 0.6931471805599453
MESH = pl.DeviceIdType.MESH


OFFSETS = [(dz, dx) for dz in (0, 1, 7, 2, 6, 3, 5, 4) for dx in (0, 1, 3, 2)]
NEAR = (1, 2, 3, 4, 8)


def shifted(me, offset):
    z, x = me // NX, lax.rem(me, NX)
    return lax.rem(z + offset[0], NZ) * NX + lax.rem(x + offset[1], NX)


def back(offset):
    return ((NZ - offset[0]) % NZ, (NX - offset[1]) % NX)


def parts_of(value):
    high = value.astype(BF).astype(F32)
    rest = value - high
    middle = rest.astype(BF).astype(F32)
    return high, middle, rest - middle


def kernel(
    *refs,
):
    hbm, refs = refs[:10], refs[10:]
    result, refs = refs[0], refs[1:]
    local, refs = refs[:10], refs[10:]
    blocks, pick, factors, weights, terms, scale, shift, discount, set_pd, own_pd = local
    (
        tiles, shocked, flat, scales, shifts, side0, side1, stage00, stage01, stage10, stage11, members_ref, coef_row, coefs, sums,
        outbox, inbox, near_out, near_in,
        load_sems, send_sems, tile_sems, out_sems, in_sems, near_send, near_recv,
    ) = refs
    sides = [side0, side1]
    staged = [[stage00, stage01], [stage10, stage11]]
    pa = lax.axis_index("pa")
    sa = lax.axis_index("sa")
    loads = [pltpu.make_async_copy(hbm[i], local[i], load_sems.at[i]) for i in range(10)]
    for load in loads:
        load.start()

    barrier = pltpu.get_barrier_semaphore()
    for k in NEAR:
        pl.semaphore_signal(barrier, inc=1, device_id={"pa": shifted(pa, OFFSETS[k])}, device_id_type=MESH)
    for hop in range(1, NSA):
        pl.semaphore_signal(barrier, inc=1, device_id={"sa": lax.rem(sa + hop, NSA)}, device_id_type=MESH)

    for i in (0, 3, 4, 8, 9):
        loads[i].wait()

    coef_row[...] = jnp.zeros_like(coef_row)
    coef_row[0:1, 0:16] = set_pd[...]
    coef_row[0:1, 16:32] = set_pd[...]
    coef_row[0:1, 32:48] = own_pd[...]
    coef_row[0:1, 48:64] = own_pd[...]
    coef = coef_row[0:1, :]
    ends = []
    running = jnp.int32(0)
    for m in range(SETS):
        running = running + blocks[m]
        ends.append(running)
    row = lax.broadcasted_iota(jnp.int32, (16, LANES), 0)
    for half in range(2):
        block = 2 * pa + half
        owner = jnp.int32(0)
        for end in ends:
            owner = owner + jnp.where(end <= block, 1, 0).astype(jnp.int32)
        lanes = slice(half * LANES, (half + 1) * LANES)
        notional = terms[0:1, lanes].astype(F32)
        strike = parts_of(terms[1:2, lanes].astype(F32) * LOG2E)
        rows = [*strike, notional, jnp.full((1, LANES), owner.astype(F32))]
        if half == 0:
            rows.extend(parts_of(coef))
        block_rows = jnp.zeros((16, LANES), F32)
        for i, value in enumerate(rows):
            block_rows = jnp.where(row == i, value, block_rows)
        tiles[0, half, 0:K] = weights[:, lanes]
        tiles[0, half, K:ROWS] = block_rows.astype(BF)

    for i in (1, 2, 5, 6, 7):
        loads[i].wait()
    for k in range(K):
        flat[k * DATES:(k + 1) * DATES, :] = factors[k].astype(F32)
    ones = jnp.where(lax.broadcasted_iota(jnp.int32, (K, LANES), 0) < 3, 1.0, 0.0).astype(BF)
    none = jnp.zeros((K, LANES), BF)
    for s in range(2):
        which = pick[s]
        scales[s] = jnp.broadcast_to(scale[pl.ds(which, 1), :], (LANES, K)).T
        shifts[s] = jnp.broadcast_to(shift[pl.ds(which, 1), :], (LANES, K)).T

    def shock(j):
        for g in range(4 * j, 4 * j + 4):
            s, d = g // DATES, g % DATES
            base = flat[pl.ds(d, K, stride=DATES), :]
            value = (scales[s] * base + shifts[s]).astype(BF).astype(F32) * LOG2E
            high = value.astype(BF)
            shocked[g, 0:K] = high
            shocked[g, K:2 * K] = ones
            shocked[g, 2 * K:3 * K] = (value - high.astype(F32)).astype(BF)
            shocked[g, 3 * K:4 * K] = none

    for j in range(2):
        shock(j)

    pl.semaphore_wait(barrier, len(NEAR) + NSA - 1)

    def tile_copy(source, k, target):
        return pltpu.make_async_remote_copy(
            src_ref=tiles.at[source], dst_ref=tiles.at[k], send_sem=send_sems.at[k], recv_sem=tile_sems.at[k],
            device_id={"pa": target}, device_id_type=MESH,
        )

    def arrived(k):
        tile_copy(k, k, pa).wait_recv()

    def pass_on(source, k):
        odd = lax.rem(k // NX, 2)
        target = lax.rem(pa // NX + 1 + (NZ - 2) * odd, NZ) * NX + lax.rem(pa, NX)
        tile_copy(source, k, target).start()

    for k in NEAR:
        tile_copy(0, k, shifted(pa, back(OFFSETS[k]))).start()

    def members(s):
        halves = []
        for half in range(2):
            info = tiles[s, half, K:ROWS].astype(F32)
            ids = lax.broadcasted_iota(jnp.int32, (SETS, LANES), 0).astype(F32)
            halves.append(jnp.where(ids == info[4:5, :], info[3:4, :], 0.0).astype(BF))
        return jnp.concatenate(halves, 1)

    def prepare(s, slot):
        for half in range(2):
            tile = jnp.concatenate([tiles[s, half], jnp.zeros((LANES - ROWS, LANES), BF)], 0)
            sides[slot][half * LANES:(half + 1) * LANES] = tile.T

    def softplus2(x):
        y = lax.log2(1.0 + lax.exp2(jnp.minimum(x, 100.0)))
        return jnp.maximum(y, x).astype(BF)

    def body(levels, nets):
        def push_shocked(q, j):
            g = (2 * (j % STEPS) + q) * 2
            both = jnp.concatenate([shocked[g], shocked[g + 1]], 1)
            pltpu.matmul_push_rhs(both, staging_register=0, mxu_index=q)

        def level(q, j, p, slot):
            side = sides[slot][p * PIECE:(p + 1) * PIECE]
            pltpu.matmul_acc_lhs(
                levels[q][j % 2][p], jnp.concatenate([side, side], 1), load_staged_rhs=0 if p == 0 else None
            )

        def net(q, j, chosen):
            values = staged[q][j % 2]
            pltpu.matmul_push_rhs(jnp.concatenate([values[0], values[1]], 1), staging_register=1, mxu_index=q)
            pltpu.matmul_acc_lhs(nets[q][j], chosen, load_staged_rhs=1)

        for q in range(2):
            for acc in nets[q]:
                pltpu.matmul_pop(acc)
            for r in range(2):
                for p in range(PIECES):
                    pltpu.matmul_pop(levels[q][r][p])
        prepare(0, 0)
        for j in range(2):
            for q in range(2):
                push_shocked(q, j)
                for p in range(PIECES):
                    level(q, j, p, 0)

        def shard(s, parity, chosen, before, first=False, last=False, finish=None):
            for j in range(STEPS):
                if first and j == 4:
                    arrived(1)
                    pass_on(1, 5)
                    pass_on(1, 9)
                if not last and j == (4 if first else 0):
                    prepare(s + 1, 1 - parity)
                slot = parity if j + 2 < STEPS else 1 - parity
                ahead = not last or j + 2 < STEPS
                if first and j + 2 < STEPS:
                    shock(j + 2)
                if ahead:
                    for q in range(2):
                        push_shocked(q, j + 2)
                for p in range(PIECES):
                    for q in range(2):
                        x = pltpu.matmul_pop(levels[q][j % 2][p])
                        if ahead:
                            level(q, j + 2, p, slot)
                        value = softplus2(x)
                        for h in range(2):
                            staged[q][j % 2][h, p * PIECE:(p + 1) * PIECE] = value[:, h * LANES:(h + 1) * LANES]
                if j or not first:
                    for q in range(2):
                        net(q, (j - 1) % STEPS, chosen if j else before)
                if last and j >= 2:
                    finish(j - 2)

        chosen = members(0)
        shard(0, 0, chosen, None, first=True)
        members_ref[...] = chosen

        def pair_of_shards(i, carry):
            arrived(2 * i + 2)
            arrived(2 * i + 3)

            @pl.when(i == 0)
            def _():
                for k in (2, 3):
                    pass_on(k, k + 4)
                    pass_on(k, k + 8)

            @pl.when(jnp.logical_and(i >= 1, i <= 10))
            def _():
                for k in (2 * i + 2, 2 * i + 3):
                    pass_on(k, k + 8)

            before = members_ref[...]
            for parity in (1, 0):
                s = 2 * i + 2 - parity
                chosen = members(s)
                shard(s, parity, chosen, before)
                before = chosen
            members_ref[...] = before
            return carry

        lax.fori_loop(0, NPA // 2 - 1, pair_of_shards, 0)
        for k in range(NPA):
            info = tiles[k, 0, K:ROWS].astype(F32)
            coefs[pl.ds(shifted(pa, OFFSETS[k]), 1), :] = info[5:6, :] + info[6:7, :] + info[7:8, :]

        lane = lax.broadcasted_iota(jnp.int32, (SETS, LANES), 1)
        sums[...] = jnp.zeros_like(sums)

        def finish(j):
            partial = sums[...]
            for q in range(2):
                netted = pltpu.matmul_pop(nets[q][j])
                for h in range(2):
                    g = (2 * j + q) * 2 + h
                    d = g % DATES
                    exposure = netted[:, h * LANES:(h + 1) * LANES] * (0.0625 * LN2) * discount[d:d + 1, :].astype(F32)
                    positive = jnp.sum(jnp.maximum(exposure, 0.0), axis=1, keepdims=True)
                    negative = jnp.sum(jnp.minimum(exposure, 0.0), axis=1, keepdims=True)
                    partial = jnp.where(lane == g, positive, partial)
                    partial = jnp.where(lane == GROUPS + g, negative, partial)
            sums[...] = partial

        chosen = members(NPA - 1)
        shard(NPA - 1, 1, chosen, members_ref[...], last=True, finish=finish)
        for q in range(2):
            net(q, STEPS - 1, chosen)
        finish(STEPS - 2)
        finish(STEPS - 1)

    acc = lambda q, m: pltpu.ACC(q)((m, 256), F32)
    pl.run_scoped(
        body,
        [[[acc(q, PIECE) for _ in range(PIECES)] for _ in range(2)] for q in range(2)],
        [[acc(q, SETS) for _ in range(STEPS)] for q in range(2)],
    )

    partial = sums[...] * (1.0 / (NPA * LANES))
    totals = jnp.sum(partial * coefs[...], axis=0, keepdims=True)
    rows = partial + pltpu.roll(jnp.broadcast_to(totals, (8, LANES)), 64, 1)[0:1, :]
    for n in range(SETS):
        outbox[n] = rows[n:n + 1, :]

    def row_copy(k, target):
        return pltpu.make_async_remote_copy(
            src_ref=outbox.at[target], dst_ref=inbox.at[k], send_sem=out_sems.at[k], recv_sem=in_sems.at[k],
            device_id={"pa": target}, device_id_type=MESH,
        )

    for k in range(NPA - 1, 0, -1):
        row_copy(k, shifted(pa, OFFSETS[k])).start()
    inbox[0] = outbox[pa]
    for k in range(1, NPA):
        row_copy(k, shifted(pa, OFFSETS[k])).wait_recv()
    mine = jnp.sum(inbox[...], axis=0)

    lane = lax.broadcasted_iota(jnp.int32, (1, LANES), 1)
    weighted = mine * coef
    first = lax.rem(lane // DATES, 2) == 0
    upper = lane >= 64

    near_out[...] = weighted

    def near_copy(hop, target):
        return pltpu.make_async_remote_copy(
            src_ref=near_out, dst_ref=near_in.at[hop], send_sem=near_send.at[hop], recv_sem=near_recv.at[hop],
            device_id={"sa": target}, device_id_type=MESH,
        )

    for hop in range(1, NSA):
        near_copy(hop, lax.rem(sa + hop, NSA)).start()
    near_in[0] = weighted

    def lane_sum(value, mask):
        return jnp.sum(jnp.where(mask, value, 0.0), axis=1, keepdims=True)

    adjust = [lane_sum(weighted, first), lane_sum(weighted, jnp.logical_not(first))]
    total = [
        lane_sum(mine, jnp.logical_and(first, upper)),
        lane_sum(mine, jnp.logical_and(jnp.logical_not(first), upper)),
    ]

    for hop in range(1, NSA):
        near_copy(hop, lax.rem(sa + hop, NSA)).wait_recv()
    mean = jnp.sum(jnp.sum(near_in[...], axis=0), axis=1, keepdims=True) / (2 * NSA)
    row = mine
    for i, value in enumerate([adjust[0] - mean, adjust[1] - mean, *total]):
        row = jnp.where(lane == 64 + i, value, row)
    result[...] = row

    for k in range(1, NPA):
        tile_copy(0, k, pa).wait_send()
        row_copy(k, shifted(pa, OFFSETS[k])).wait_send()
    for hop in range(1, NSA):
        near_copy(hop, sa).wait_send()


def spread(row, profile_out, xva_out, total_out):
    values = row[...]
    for sign in range(2):
        for s in range(2):
            start = sign * 32 + s * 16
            profile_out[sign, s:s + 1, :] = values[:, start:start + DATES]
    xva_out[...] = values[:, 64:66]
    total_out[...] = values[:, 66:68]


def on_device(
    factors, trade_weights, payoff_terms, set_blocks, shock_pick, shock_scale, shock_shift, discount, set_pd, own_pd
):
    vmem = pl.BlockSpec(memory_space=pltpu.VMEM)
    arrays = [
        set_blocks, shock_pick, factors, trade_weights, payoff_terms, shock_scale, shock_shift, discount, set_pd,
        own_pd.reshape(1, DATES),
    ]
    row = pl.pallas_call(
        kernel,
        out_shape=jax.ShapeDtypeStruct((1, LANES), F32),
        in_specs=[pl.BlockSpec(memory_space=pl.ANY)] * 10,
        out_specs=vmem,
        scratch_shapes=[
            *(pltpu.SMEM(a.shape, a.dtype) for a in arrays[:2]),
            *(pltpu.VMEM(a.shape, a.dtype) for a in arrays[2:]),
            pltpu.VMEM((NPA, 2, ROWS, LANES), BF),
            pltpu.VMEM((GROUPS, 256, LANES), BF),
            pltpu.VMEM((K * DATES, LANES), F32),
            *(pltpu.VMEM((2, K, LANES), F32) for _ in range(2)),
            *(pltpu.VMEM((256, LANES), BF) for _ in range(2)),
            *(pltpu.VMEM((2, 256, LANES), BF) for _ in range(4)),
            pltpu.VMEM((SETS, 256), BF),
            pltpu.VMEM((8, LANES), F32),
            pltpu.VMEM((SETS, LANES), F32),
            pltpu.VMEM((SETS, LANES), F32),
            pltpu.VMEM((SETS, 1, LANES), F32),
            pltpu.VMEM((NPA, 1, LANES), F32),
            pltpu.VMEM((1, LANES), F32),
            pltpu.VMEM((NSA, 1, LANES), F32),
            pltpu.SemaphoreType.DMA((10,)),
            pltpu.SemaphoreType.DMA((NPA,)),
            pltpu.SemaphoreType.DMA((NPA,)),
            pltpu.SemaphoreType.DMA((NPA,)),
            pltpu.SemaphoreType.DMA((NPA,)),
            pltpu.SemaphoreType.DMA((NSA,)),
            pltpu.SemaphoreType.DMA((NSA,)),
        ],
        compiler_params=pltpu.CompilerParams(
            collective_id=0, has_side_effects=True, vmem_limit_bytes=60 << 20,
        ),
        name="valuation",
    )(*arrays)
    profile, xva, total = pl.pallas_call(
        spread,
        out_shape=(
            jax.ShapeDtypeStruct((2, 2, DATES), F32),
            jax.ShapeDtypeStruct((1, 2), F32),
            jax.ShapeDtypeStruct((1, 2), F32),
        ),
        in_specs=[vmem],
        out_specs=(vmem, vmem, vmem),
        name="spread",
    )(row)
    return profile.transpose(0, 2, 1).reshape(2, 1, DATES, 2), xva, total.reshape(2)


def solution(mesh):
    return jax.shard_map(
        on_device,
        mesh=mesh,
        in_specs=(
            P(None, None, "pa"), P(None, "pa"), P(None, "pa"), P(), P("sa"), P(), P(), P(None, "pa"),
            P("pa", None), P(),
        ),
        out_specs=(P(None, "pa", None, "sa"), P("pa", "sa"), P("sa")),
        check_vma=False,
    )
```

```python
import functools

import jax
import jax.numpy as jnp
from jax import lax
from jax.experimental import pallas as pl
from jax.experimental.pallas import tpu as pltpu
from jax.sharding import PartitionSpec as P

BF = jnp.bfloat16
F32 = jnp.float32
K = 64
SETS = 32
DATES = 16
LANES = 128
ROWS = 80
GROUPS = 32
STEPS = 8
PIECE = 128
PIECES = 2
NZ, NX, NPA, NSA = 8, 4, 32, 8
LOG2E = 1.4426950408889634
LN2 = 0.6931471805599453
MESH = pl.DeviceIdType.MESH


OFFSETS = [(dz, dx) for dz in (0, 1, 7, 2, 6, 3, 5, 4) for dx in (0, 1, 3, 2)]
NEAR = (1, 2, 3, 4, 8)


def shifted(me, offset):
    z, x = me // NX, lax.rem(me, NX)
    return lax.rem(z + offset[0], NZ) * NX + lax.rem(x + offset[1], NX)


def back(offset):
    return ((NZ - offset[0]) % NZ, (NX - offset[1]) % NX)


def parts_of(value):
    high = value.astype(BF).astype(F32)
    rest = value - high
    middle = rest.astype(BF).astype(F32)
    return high, middle, rest - middle


def kernel(
    *refs,
):
    hbm, refs = refs[:10], refs[10:]
    result, refs = refs[0], refs[1:]
    local, refs = refs[:10], refs[10:]
    blocks, pick, factors, weights, terms, scale, shift, discount, set_pd, own_pd = local
    (
        tiles, shocked, flat, scales, shifts, side0, side1, stage00, stage01, stage10, stage11, members_ref, coef_row, coefs, sums,
        outbox, inbox, near_out, near_in,
        load_sems, send_sems, tile_sems, out_sems, in_sems, near_send, near_recv,
    ) = refs
    sides = [side0, side1]
    staged = [[stage00, stage01], [stage10, stage11]]
    pa = lax.axis_index("pa")
    sa = lax.axis_index("sa")
    loads = [pltpu.make_async_copy(hbm[i], local[i], load_sems.at[i]) for i in range(10)]
    for load in loads:
        load.start()

    barrier = pltpu.get_barrier_semaphore()
    for k in NEAR:
        pl.semaphore_signal(barrier, inc=1, device_id={"pa": shifted(pa, OFFSETS[k])}, device_id_type=MESH)
    for hop in range(1, NSA):
        pl.semaphore_signal(barrier, inc=1, device_id={"sa": lax.rem(sa + hop, NSA)}, device_id_type=MESH)

    for i in (0, 3, 4, 8, 9):
        loads[i].wait()

    coef_row[...] = jnp.zeros_like(coef_row)
    coef_row[0:1, 0:16] = set_pd[...]
    coef_row[0:1, 16:32] = set_pd[...]
    coef_row[0:1, 32:48] = own_pd[...]
    coef_row[0:1, 48:64] = own_pd[...]
    coef = coef_row[0:1, :]
    ends = []
    running = jnp.int32(0)
    for m in range(SETS):
        running = running + blocks[m]
        ends.append(running)
    row = lax.broadcasted_iota(jnp.int32, (16, LANES), 0)
    for half in range(2):
        block = 2 * pa + half
        owner = jnp.int32(0)
        for end in ends:
            owner = owner + jnp.where(end <= block, 1, 0).astype(jnp.int32)
        lanes = slice(half * LANES, (half + 1) * LANES)
        notional = terms[0:1, lanes].astype(F32)
        strike = parts_of(terms[1:2, lanes].astype(F32) * LOG2E)
        rows = [*strike, notional, jnp.full((1, LANES), owner.astype(F32))]
        if half == 0:
            rows.extend(parts_of(coef))
        block_rows = jnp.zeros((16, LANES), F32)
        for i, value in enumerate(rows):
            block_rows = jnp.where(row == i, value, block_rows)
        tiles[0, half, 0:K] = weights[:, lanes]
        tiles[0, half, K:ROWS] = block_rows.astype(BF)

    for i in (1, 5, 6):
        loads[i].wait()
    for s in range(2):
        which = pick[s]
        scales[s] = jnp.broadcast_to(scale[pl.ds(which, 1), :], (LANES, K)).T
        shifts[s] = jnp.broadcast_to(shift[pl.ds(which, 1), :], (LANES, K)).T

    pl.semaphore_wait(barrier, len(NEAR) + NSA - 1)

    def tile_copy(source, k, target):
        return pltpu.make_async_remote_copy(
            src_ref=tiles.at[source], dst_ref=tiles.at[k], send_sem=send_sems.at[k], recv_sem=tile_sems.at[k],
            device_id={"pa": target}, device_id_type=MESH,
        )

    def arrived(k):
        tile_copy(k, k, pa).wait_recv()

    def pass_on(source, k):
        odd = lax.rem(k // NX, 2)
        target = lax.rem(pa // NX + 1 + (NZ - 2) * odd, NZ) * NX + lax.rem(pa, NX)
        tile_copy(source, k, target).start()

    for k in NEAR:
        tile_copy(0, k, shifted(pa, back(OFFSETS[k]))).start()

    for i in (2, 7):
        loads[i].wait()
    for k in range(K):
        flat[k * DATES:(k + 1) * DATES, :] = factors[k].astype(F32)
    ones = jnp.where(lax.broadcasted_iota(jnp.int32, (K, LANES), 0) < 3, 1.0, 0.0).astype(BF)
    none = jnp.zeros((K, LANES), BF)

    def shock(j):
        for g in range(4 * j, 4 * j + 4):
            s, d = g // DATES, g % DATES
            base = flat[pl.ds(d, K, stride=DATES), :]
            value = (scales[s] * base + shifts[s]).astype(BF).astype(F32) * LOG2E
            high = value.astype(BF)
            shocked[g, 0:K] = high
            shocked[g, K:2 * K] = ones
            shocked[g, 2 * K:3 * K] = (value - high.astype(F32)).astype(BF)
            shocked[g, 3 * K:4 * K] = none

    for j in range(2):
        shock(j)

    def members(s):
        halves = []
        for half in range(2):
            info = tiles[s, half, K:ROWS].astype(F32)
            ids = lax.broadcasted_iota(jnp.int32, (SETS, LANES), 0).astype(F32)
            halves.append(jnp.where(ids == info[4:5, :], info[3:4, :], 0.0).astype(BF))
        return jnp.concatenate(halves, 1)

    def prepare(s, slot):
        for half in range(2):
            tile = jnp.concatenate([tiles[s, half], jnp.zeros((LANES - ROWS, LANES), BF)], 0)
            sides[slot][half * LANES:(half + 1) * LANES] = tile.T

    def softplus2(x):
        y = lax.log2(1.0 + lax.exp2(jnp.minimum(x, 100.0)))
        return jnp.maximum(y, x).astype(BF)

    def body(levels, nets):
        def push_shocked(q, j):
            g = (2 * (j % STEPS) + q) * 2
            both = jnp.concatenate([shocked[g], shocked[g + 1]], 1)
            pltpu.matmul_push_rhs(both, staging_register=0, mxu_index=q)

        def level(q, j, p, slot):
            side = sides[slot][p * PIECE:(p + 1) * PIECE]
            pltpu.matmul_acc_lhs(
                levels[q][j % 2][p], jnp.concatenate([side, side], 1), load_staged_rhs=0 if p == 0 else None
            )

        def net(q, j, chosen):
            values = staged[q][j % 2]
            pltpu.matmul_push_rhs(jnp.concatenate([values[0], values[1]], 1), staging_register=1, mxu_index=q)
            pltpu.matmul_acc_lhs(nets[q][j], chosen, load_staged_rhs=1)

        for q in range(2):
            for acc in nets[q]:
                pltpu.matmul_pop(acc)
            for r in range(2):
                for p in range(PIECES):
                    pltpu.matmul_pop(levels[q][r][p])
        prepare(0, 0)
        for j in range(2):
            for q in range(2):
                push_shocked(q, j)
                for p in range(PIECES):
                    level(q, j, p, 0)

        def shard(s, parity, chosen, before, first=False, last=False, finish=None):
            for j in range(STEPS):
                if first and j == 4:
                    arrived(1)
                    pass_on(1, 5)
                    pass_on(1, 9)
                if not last and j == (4 if first else 0):
                    prepare(s + 1, 1 - parity)
                slot = parity if j + 2 < STEPS else 1 - parity
                ahead = not last or j + 2 < STEPS
                if first and j + 2 < STEPS:
                    shock(j + 2)
                if ahead:
                    for q in range(2):
                        push_shocked(q, j + 2)
                for p in range(PIECES):
                    for q in range(2):
                        x = pltpu.matmul_pop(levels[q][j % 2][p])
                        if ahead:
                            level(q, j + 2, p, slot)
                        value = softplus2(x)
                        for h in range(2):
                            staged[q][j % 2][h, p * PIECE:(p + 1) * PIECE] = value[:, h * LANES:(h + 1) * LANES]
                if j or not first:
                    for q in range(2):
                        net(q, (j - 1) % STEPS, chosen if j else before)
                if last and j >= 2:
                    finish(j - 2)

        chosen = members(0)
        shard(0, 0, chosen, None, first=True)
        members_ref[...] = chosen

        def pair_of_shards(i, carry):
            arrived(2 * i + 2)
            arrived(2 * i + 3)

            @pl.when(i == 0)
            def _():
                for k in (2, 3):
                    pass_on(k, k + 4)
                    pass_on(k, k + 8)

            @pl.when(jnp.logical_and(i >= 1, i <= 10))
            def _():
                for k in (2 * i + 2, 2 * i + 3):
                    pass_on(k, k + 8)

            before = members_ref[...]
            for parity in (1, 0):
                s = 2 * i + 2 - parity
                chosen = members(s)
                shard(s, parity, chosen, before)
                before = chosen
            members_ref[...] = before
            return carry

        lax.fori_loop(0, NPA // 2 - 1, pair_of_shards, 0)
        for k in range(NPA):
            info = tiles[k, 0, K:ROWS].astype(F32)
            coefs[pl.ds(shifted(pa, OFFSETS[k]), 1), :] = info[5:6, :] + info[6:7, :] + info[7:8, :]

        lane = lax.broadcasted_iota(jnp.int32, (SETS, LANES), 1)
        sums[...] = jnp.zeros_like(sums)

        def finish(j):
            partial = sums[...]
            for q in range(2):
                netted = pltpu.matmul_pop(nets[q][j])
                for h in range(2):
                    g = (2 * j + q) * 2 + h
                    d = g % DATES
                    exposure = netted[:, h * LANES:(h + 1) * LANES] * (0.0625 * LN2) * discount[d:d + 1, :].astype(F32)
                    positive = jnp.sum(jnp.maximum(exposure, 0.0), axis=1, keepdims=True)
                    negative = jnp.sum(jnp.minimum(exposure, 0.0), axis=1, keepdims=True)
                    partial = jnp.where(lane == g, positive, partial)
                    partial = jnp.where(lane == GROUPS + g, negative, partial)
            sums[...] = partial

        chosen = members(NPA - 1)
        shard(NPA - 1, 1, chosen, members_ref[...], last=True, finish=finish)
        for q in range(2):
            net(q, STEPS - 1, chosen)
        finish(STEPS - 2)
        finish(STEPS - 1)

    acc = lambda q, m: pltpu.ACC(q)((m, 256), F32)
    pl.run_scoped(
        body,
        [[[acc(q, PIECE) for _ in range(PIECES)] for _ in range(2)] for q in range(2)],
        [[acc(q, SETS) for _ in range(STEPS)] for q in range(2)],
    )

    partial = sums[...] * (1.0 / (NPA * LANES))
    totals = jnp.sum(partial * coefs[...], axis=0, keepdims=True)
    rows = partial + pltpu.roll(jnp.broadcast_to(totals, (8, LANES)), 64, 1)[0:1, :]
    for n in range(SETS):
        outbox[n] = rows[n:n + 1, :]

    def row_copy(k, target):
        return pltpu.make_async_remote_copy(
            src_ref=outbox.at[target], dst_ref=inbox.at[k], send_sem=out_sems.at[k], recv_sem=in_sems.at[k],
            device_id={"pa": target}, device_id_type=MESH,
        )

    for k in range(NPA - 1, 0, -1):
        row_copy(k, shifted(pa, OFFSETS[k])).start()
    inbox[0] = outbox[pa]
    for k in range(1, NPA):
        row_copy(k, shifted(pa, OFFSETS[k])).wait_recv()
    mine = jnp.sum(inbox[...], axis=0)

    lane = lax.broadcasted_iota(jnp.int32, (1, LANES), 1)
    weighted = mine * coef
    first = lax.rem(lane // DATES, 2) == 0
    upper = lane >= 64

    near_out[...] = weighted

    def near_copy(hop, target):
        return pltpu.make_async_remote_copy(
            src_ref=near_out, dst_ref=near_in.at[hop], send_sem=near_send.at[hop], recv_sem=near_recv.at[hop],
            device_id={"sa": target}, device_id_type=MESH,
        )

    for hop in range(1, NSA):
        near_copy(hop, lax.rem(sa + hop, NSA)).start()
    near_in[0] = weighted

    def lane_sum(value, mask):
        return jnp.sum(jnp.where(mask, value, 0.0), axis=1, keepdims=True)

    adjust = [lane_sum(weighted, first), lane_sum(weighted, jnp.logical_not(first))]
    total = [
        lane_sum(mine, jnp.logical_and(first, upper)),
        lane_sum(mine, jnp.logical_and(jnp.logical_not(first), upper)),
    ]

    for hop in range(1, NSA):
        near_copy(hop, lax.rem(sa + hop, NSA)).wait_recv()
    mean = jnp.sum(jnp.sum(near_in[...], axis=0), axis=1, keepdims=True) / (2 * NSA)
    row = mine
    for i, value in enumerate([adjust[0] - mean, adjust[1] - mean, *total]):
        row = jnp.where(lane == 64 + i, value, row)
    result[...] = row

    for k in range(1, NPA):
        tile_copy(0, k, pa).wait_send()
        row_copy(k, shifted(pa, OFFSETS[k])).wait_send()
    for hop in range(1, NSA):
        near_copy(hop, sa).wait_send()


def spread(row, profile_out, xva_out, total_out):
    values = row[...]
    for sign in range(2):
        for s in range(2):
            start = sign * 32 + s * 16
            profile_out[sign, s:s + 1, :] = values[:, start:start + DATES]
    xva_out[...] = values[:, 64:66]
    total_out[...] = values[:, 66:68]


def on_device(
    factors, trade_weights, payoff_terms, set_blocks, shock_pick, shock_scale, shock_shift, discount, set_pd, own_pd
):
    vmem = pl.BlockSpec(memory_space=pltpu.VMEM)
    arrays = [
        set_blocks, shock_pick, factors, trade_weights, payoff_terms, shock_scale, shock_shift, discount, set_pd,
        own_pd.reshape(1, DATES),
    ]
    row = pl.pallas_call(
        kernel,
        out_shape=jax.ShapeDtypeStruct((1, LANES), F32),
        in_specs=[pl.BlockSpec(memory_space=pl.ANY)] * 10,
        out_specs=vmem,
        scratch_shapes=[
            *(pltpu.SMEM(a.shape, a.dtype) for a in arrays[:2]),
            *(pltpu.VMEM(a.shape, a.dtype) for a in arrays[2:]),
            pltpu.VMEM((NPA, 2, ROWS, LANES), BF),
            pltpu.VMEM((GROUPS, 256, LANES), BF),
            pltpu.VMEM((K * DATES, LANES), F32),
            *(pltpu.VMEM((2, K, LANES), F32) for _ in range(2)),
            *(pltpu.VMEM((256, LANES), BF) for _ in range(2)),
            *(pltpu.VMEM((2, 256, LANES), BF) for _ in range(4)),
            pltpu.VMEM((SETS, 256), BF),
            pltpu.VMEM((8, LANES), F32),
            pltpu.VMEM((SETS, LANES), F32),
            pltpu.VMEM((SETS, LANES), F32),
            pltpu.VMEM((SETS, 1, LANES), F32),
            pltpu.VMEM((NPA, 1, LANES), F32),
            pltpu.VMEM((1, LANES), F32),
            pltpu.VMEM((NSA, 1, LANES), F32),
            pltpu.SemaphoreType.DMA((10,)),
            pltpu.SemaphoreType.DMA((NPA,)),
            pltpu.SemaphoreType.DMA((NPA,)),
            pltpu.SemaphoreType.DMA((NPA,)),
            pltpu.SemaphoreType.DMA((NPA,)),
            pltpu.SemaphoreType.DMA((NSA,)),
            pltpu.SemaphoreType.DMA((NSA,)),
        ],
        compiler_params=pltpu.CompilerParams(
            collective_id=0, has_side_effects=True, vmem_limit_bytes=60 << 20,
        ),
        name="valuation",
    )(*arrays)
    profile, xva, total = pl.pallas_call(
        spread,
        out_shape=(
            jax.ShapeDtypeStruct((2, 2, DATES), F32),
            jax.ShapeDtypeStruct((1, 2), F32),
            jax.ShapeDtypeStruct((1, 2), F32),
        ),
        in_specs=[vmem],
        out_specs=(vmem, vmem, vmem),
        name="spread",
    )(row)
    return profile.transpose(0, 2, 1).reshape(2, 1, DATES, 2), xva, total.reshape(2)


def solution(mesh):
    return jax.shard_map(
        on_device,
        mesh=mesh,
        in_specs=(
            P(None, None, "pa"), P(None, "pa"), P(None, "pa"), P(), P("sa"), P(), P(), P(None, "pa"),
            P("pa", None), P(),
        ),
        out_specs=(P(None, "pa", None, "sa"), P("pa", "sa"), P("sa")),
        check_vma=False,
    )
```
